512 devices in a mesh: fsdp: 64 (over y, x, core), tp: 8 (over z).
Axes of the slice: x: 4, y: 8, z: 8, core: 2. Of those that a mesh axis runs over, the one named last changes fastest.
Arguments:
- grads: bfloat16 [128, 128, 8192], P('tp', None, 'fsdp'), may hold values from -60 to 60
- momentum: bfloat16 [128, 128, 8192], P('tp', None, 'fsdp'), may hold values from -6 to 6
- owner_table: int32 [128, 1], P('tp'), may hold values from 0 to 63; in each aligned block of 16 rows (0 to 15, 16 to 31, ...) at most 2 rows name the same one
- pool_map: int32 [8, 16], P('tp'), may hold values from 0 to 15, each once within a row
Outputs:
- new_momentum: bfloat16 [128, 128, 8192], P('tp', None, 'fsdp')
- pool_update: bfloat16 [128, 128, 8192], P('tp', None, 'fsdp')
- slot_rms: float32 [8, 128], P('tp', 'fsdp')
The draws below stay inside these ranges and needn't reach their ends.
Inputs may be any that keep to these rules, and one draw needn't show every extreme that they name: `owner_table`: within each aligned block of 16 rows (the head blocks of one index of tp) no owner is named more than 2 times. `pool_map`: each row is a permutation of 0 to 15.
All inputs are finite; a program needn't handle non-finite values.
Results may differ from the reference program's by a relative error of at most 0.0058.
Values may be sent and summed in bfloat16 or wider, within the bound.
A program may use at most 64 MiB of HBM per device.

```python
import math
import jax
import jax.numpy as jnp
import numpy as np
from jax import lax

D = 8192
HEAD = 128
NB_ROW = 16
CAP = 2
ITERS = 3
NBLK = 128
N_FSDP = 64
N_TP = 8


def draw_grads(key, part):
    keys = jax.random.split(jax.random.fold_in(key, 17), 3)
    row_scale = jnp.exp(jax.random.uniform(keys[0], (NBLK, HEAD, 1), jnp.float32, math.log(0.3), math.log(3.0)))
    col_scale = jnp.exp(jax.random.uniform(keys[1], (NBLK, 1, D), jnp.float32, math.log(0.3), math.log(3.0)))
    values = jnp.clip(jax.random.normal(keys[2], (NBLK, HEAD, D), jnp.float32), -6.0, 6.0)
    return (values * row_scale * col_scale).astype(jnp.bfloat16)


def shard_levels(rng, shape, shards, least, high):
    def one(dim, parts):
        draws = jax.random.uniform(jax.random.fold_in(jax.random.fold_in(rng, 6), dim), (parts,), jnp.float32, least / len(shards), high / len(shards))
        return jnp.repeat(jnp.exp(draws), shape[dim] // parts).reshape((-1,) + (1,) * (len(shape) - dim - 1))

    level = one(*shards[0])
    for cut in shards[1:]:
        level = level * one(*cut)
    return level


def shared_out(stream_key, own, number, rows, number_of, top, limit, slope):
    ranking = jax.random.permutation(stream_key, number_of)
    heavy_load, usual = shares(number_of, rows * top, limit, slope, True), shares(number_of, rows * top, limit, slope, False)
    places = jnp.arange(number_of)

    def named(tallies, offset_by):
        used = int((tallies > 0).sum())
        fixed = max(1, used // 4)
        moved = fixed + (places - fixed + offset_by * (used - fixed)) % max(1, number_of - fixed)
        return jnp.zeros((number_of,), jnp.int32).at[ranking[jnp.where(places < fixed, places, moved)]].set(jnp.asarray(tallies, jnp.int32))

    tallies = jnp.where(number % 4 == 0, named(heavy_load, number // 4), named(usual, number - number // 4 - 1))
    mixed = jax.random.permutation(jax.random.fold_in(own, 3), number_of)
    source_of, taker = mixed[0:number_of // 2 * 2:2], mixed[1:number_of // 2 * 2:2]
    margin = jnp.minimum(tallies[source_of] - 1, limit - tallies[taker]) // 2
    margin = jnp.where((source_of == ranking[0]) | (taker == ranking[0]) | (tallies[taker] == 0), 0, jnp.maximum(margin, 0))
    moved = jax.random.randint(jax.random.fold_in(own, 4), (number_of // 2,), 0, 1 << 20) % (margin + 1)
    tallies = tallies.at[source_of].add(-moved).at[taker].add(moved)
    members = jnp.searchsorted(jnp.cumsum(tallies), jnp.arange(rows * top), side="right").astype(jnp.int32)
    grid = members.reshape(top, rows).T
    grid = grid[jax.random.permutation(jax.random.fold_in(own, 1), rows)]
    offset_by = jax.random.randint(jax.random.fold_in(own, 2), (rows, 1), 0, top)
    return jnp.take_along_axis(grid, (jnp.arange(top)[None, :] + offset_by) % top, axis=1)


def shares(number_of, total, limit, slope, full):
    loads = [(1 << 20) // math.isqrt(rank ** slope) + 1 for rank in range(1, number_of + 1)]
    largest = limit if full else min(limit, max(-(-total // number_of), total * loads[0] // sum(loads)))
    least = 1 if total - largest >= number_of - 1 else 0
    holding, rest = [largest] + [least] * (number_of - 1), total - largest - least * (number_of - 1)
    while rest > 0:
        candidates = [i for i in range(1, number_of) if holding[i] < largest] or [i for i in range(1, number_of) if holding[i] < limit]
        whole, budget = sum([loads[i] for i in candidates]), rest
        for i in candidates:
            more = min(limit - holding[i], max(1, budget * loads[i] // whole), rest)
            holding[i] = holding[i] + more
            rest = rest - more
    return np.array(holding)


def normal_values(rng, extent, spread, most, pieces=(), held_as=jnp.bfloat16):
    array = spread * jax.random.normal(rng, extent, jnp.float32)
    if pieces:
        array = array * shard_levels(rng, extent, pieces, -0.22, 0.18)
    return jnp.clip(array, -most, most).astype(held_as)


def setup_inputs(seed: int = 0) -> dict:
    key_of = jax.random.split(jax.random.key(seed), 5)
    grads = draw_grads(jax.random.fold_in(key_of[4], 71), 0)
    momentum = normal_values(key_of[1], (NBLK, HEAD, D), 1.0, 6.0, ((0, 8), (2, 64)))
    owner_table_keys = jax.random.split(jax.random.fold_in(key_of[2], 1), NBLK // NB_ROW)
    owner_table_turns = jax.random.permutation(jax.random.fold_in(key_of[2], 3), NBLK // NB_ROW)
    owner_table = jax.vmap(lambda own, number: shared_out(jax.random.fold_in(key_of[2], 2), own, number, NB_ROW, N_FSDP, 1, CAP, 2))(owner_table_keys, owner_table_turns).reshape((NBLK, 1))
    pool_map = jax.vmap(lambda own: jax.random.permutation(own, NB_ROW))(jax.random.split(key_of[3], N_TP)).reshape((N_TP, NB_ROW)).astype(jnp.int32)
    return dict(grads=grads, momentum=momentum, owner_table=owner_table, pool_map=pool_map)


momentum_rate = 0.95
step_size = 0.8
epsilon = 1e-07
poly_linear = 3.4445
poly_cubic = -4.775
poly_quintic = 2.0315

def newton_schulz(block):
    values = block.astype(jnp.float32)
    squares = jnp.sum(values * values)
    inverse = 1.0 / (jnp.sqrt(squares) + epsilon)
    gram = jnp.dot(values, values.T, precision=lax.Precision.HIGHEST) * (inverse * inverse)
    identity = jnp.eye(gram.shape[0], dtype=jnp.float32)
    transform = identity
    for _ in range(ITERS):
        square_gram = jnp.dot(gram, gram, precision=lax.Precision.HIGHEST)
        mixed = poly_linear * identity + poly_cubic * gram + poly_quintic * square_gram
        transform = jnp.dot(mixed, transform, precision=lax.Precision.HIGHEST)
        gram = jnp.dot(mixed, jnp.dot(gram, mixed, precision=lax.Precision.HIGHEST), precision=lax.Precision.HIGHEST)
    current = jnp.dot(transform * inverse, values, precision=lax.Precision.HIGHEST)
    return (current.astype(jnp.bfloat16), squares)

def reference(grads, momentum, owner_table, pool_map):
    velocity = momentum_rate * momentum.astype(jnp.float32) + grads.astype(jnp.float32)
    new_momentum = velocity.astype(jnp.bfloat16)
    nesterov = (grads.astype(jnp.float32) + momentum_rate * velocity).astype(jnp.bfloat16)
    ortho, squares = lax.map(newton_schulz, nesterov)
    factor = step_size * 0.2 * math.sqrt(D)
    update = (-factor * ortho.astype(jnp.float32)).astype(jnp.bfloat16)
    group = NB_ROW // N_TP
    row_index = jnp.arange(NBLK, dtype=jnp.int32) // NB_ROW
    codes = pool_map.reshape(-1).astype(jnp.int32)
    target = codes // group * NB_ROW + row_index * group + codes % group
    pool_update = jnp.zeros_like(update).at[target].set(update)
    owners = owner_table.reshape(N_TP, NB_ROW).astype(jnp.int32)
    position = jnp.arange(NB_ROW, dtype=jnp.int32)
    earlier = position[None, :] < position[:, None]
    same_owner = owners[:, :, None] == owners[:, None, :]
    slots = lax.optimization_barrier(jnp.sum(jnp.logical_and(same_owner, earlier[None]), axis=-1)).astype(jnp.int32)
    place = row_index * (N_FSDP * CAP) + owners.reshape(-1) * CAP + slots.reshape(-1)
    rms_values = jnp.sqrt(squares / (HEAD * D))
    slot_rms = jnp.zeros((N_TP * N_FSDP * CAP,), jnp.float32).at[place].set(rms_values)
    return (new_momentum, pool_update, slot_rms.reshape(N_TP, N_FSDP * CAP))
```

```python
import functools
import math

import jax
import jax.numpy as jnp
from jax import lax
from jax.experimental import pallas as pl
from jax.experimental.pallas import tpu as pltpu
from jax.sharding import PartitionSpec as P

ITERS = 3
momentum_rate = 0.95
step_size = 0.8
epsilon = 1e-07
poly_linear = 3.4445
poly_cubic = -4.775
poly_quintic = 2.0315

H = 128
PACKED = H + 8
MESH = pl.DeviceIdType.MESH


def masks():
    row = lax.broadcasted_iota(jnp.int32, (H, H), 0)
    col = lax.broadcasted_iota(jnp.int32, (H, H), 1)
    return row >= col, row == col


def put_packed(ref, a, b):
    low, diag = masks()
    ref[0:H, :] = jnp.where(low, a, b)
    last = jnp.sum(jnp.where(diag, b, 0.0), axis=0, keepdims=True)
    ref[H:PACKED, :] = jnp.broadcast_to(last, (8, H))


def get_packed(ref):
    low, diag = masks()
    both = ref[0:H, :]
    other = both.T
    last = jnp.broadcast_to(ref[H : H + 1, :], (H, H))
    a = jnp.where(low, both, other)
    b = jnp.where(diag, last, jnp.where(low, other, both))
    return a, b


def dot32(a, b):
    return jnp.dot(a, b, precision=lax.Precision.HIGHEST, preferred_element_type=jnp.float32)


def newton_schulz(grams):
    _, diag = masks()
    identity = jnp.where(diag, 1.0, 0.0)
    inverses, gs, qs = [], [], [None] * len(grams)
    for g in grams:
        squares = jnp.sum(jnp.where(diag, g, 0.0), keepdims=True)
        inverse = 1.0 / (jnp.sqrt(squares) + epsilon)
        inverses.append(inverse)
        gs.append(g * (inverse * inverse))
    for it in range(ITERS):
        g2 = [dot32(g, g) for g in gs]
        ms = [poly_linear * identity + poly_cubic * g + poly_quintic * s for g, s in zip(gs, g2)]
        if it < ITERS - 1:
            right = [dot32(g, m) for g, m in zip(gs, ms)]
        qs = [m if it == 0 else dot32(m, q) for m, q in zip(ms, qs)]
        if it < ITERS - 1:
            gs = [dot32(m, r) for m, r in zip(ms, right)]
    return [q * inverse for q, inverse in zip(qs, inverses)]


def kernel(
    sizes,
    owner_ref,
    pool_ref,
    g_hbm,
    m_hbm,
    nm_hbm,
    out_hbm,
    slot_ref,
    gbuf,
    mbuf,
    nmbuf,
    nes,
    yq,
    yr,
    pk,
    r0,
    s1,
    r1,
    s2,
    r2,
    rd,
    s3,
    sd,
    gram,
    qall,
    outbuf,
    t0,
    t0r,
    t1,
    t1r,
    t2,
    t2r,
    in_sem,
    nm_sem,
    out_sem,
    z_send,
    z_recv,
    c_send,
    c_recv,
    x_send,
    x_recv,
    y_send,
    y_recv,
    t_send,
    t_recv,
    w_send,
    w_recv,
    a_send,
    a_recv,
    b_send,
    b_recv,
):
    NX, NY, NZ, NB = sizes
    NK = 2 * NX
    CH = H // NY
    f = lax.axis_index("fsdp")
    z = lax.axis_index("tp")
    k = lax.rem(f, NK)
    y = lax.div(f, NK)
    x = lax.div(k, 2)
    c = lax.rem(k, 2)

    def dev(yy, xx, cc, zz):
        return ((yy * NX + xx) * 2 + cc, zz)

    partner = dev(y, x, 1 - c, z)

    def xdev(d):
        return dev(y, lax.rem(x + d, NX), c, z)

    def ydev(d):
        return dev(lax.rem(y + d, NY), x, c, z)

    def zdev(d):
        return dev(y, x, c, lax.rem(z + d, NZ))

    def wdev(d):
        return (lax.rem(y + d, NY) * NK + z, k)

    def remote(src, dst, send, recv, device):
        return pltpu.make_async_remote_copy(
            src_ref=src, dst_ref=dst, send_sem=send, recv_sem=recv, device_id=device, device_id_type=MESH
        )

    CHUNKS = 4
    per = NB // CHUNKS
    loads = []
    for i in range(CHUNKS):
        part = pl.ds(i * per, per)
        lg = pltpu.make_async_copy(g_hbm.at[part], gbuf.at[part], in_sem.at[2 * i])
        lm = pltpu.make_async_copy(m_hbm.at[part], mbuf.at[part], in_sem.at[2 * i + 1])
        lg.start()
        lm.start()
        loads.append((lg, lm))

    barrier = pltpu.get_barrier_semaphore()

    def greet(device):
        pl.semaphore_signal(barrier, inc=1, device_id=device, device_id_type=MESH)

    for d in range(1, NZ):
        greet(zdev(d))
    for d in range(1, NY):
        greet(ydev(d))
    for d in range(1, NX):
        greet(xdev(d))
    greet(partner)

    @pl.when(k != z)
    def _():
        for d in range(NY):
            greet(wdev(d))

    codes = [pool_ref[0, j] for j in range(NB)]
    source = []
    for q in range(NB):
        at = jnp.int32(0)
        for j in range(1, NB):
            at = jnp.where(codes[j] == q, j, at)
        source.append(at)

    stores = []
    for i in range(CHUNKS):
        for cp in loads[i]:
            cp.wait()
        for j in range(i * per, (i + 1) * per):
            grad = gbuf[j].astype(jnp.float32)
            velocity = momentum_rate * mbuf[j].astype(jnp.float32) + grad
            nmbuf[j] = velocity.astype(jnp.bfloat16)
            nes[j] = (grad + momentum_rate * velocity).astype(jnp.bfloat16)
        part = pl.ds(i * per, per)
        st = pltpu.make_async_copy(nmbuf.at[part], nm_hbm.at[part], nm_sem.at[i])
        st.start()
        stores.append(st)

    for p in range(NZ):
        grams = []
        for e in range(2):
            q = 2 * p + e
            value = nes[source[q]]
            yq[q] = value
            wide = value.astype(jnp.float32)
            t0[q : q + 1, :] = jnp.sum(wide * wide, axis=0, keepdims=True)
            grams.append(
                lax.dot_general(value, value, (((1,), (1,)), ((), ())), preferred_element_type=jnp.float32)
            )
        put_packed(pk.at[p % 2, p // 2], *grams)

    pl.semaphore_wait(barrier, (NZ - 1) + (NY - 1) + (NX - 1) + 1 + jnp.where(k != z, NY, 0))

    sent = []

    def go(copy):
        copy.start()
        sent.append(copy)
        return copy

    cc = go(remote(pk.at[1 - c], r0, c_send.at[0], c_recv.at[0], partner))
    ct = go(remote(t0, t0r, c_send.at[1], c_recv.at[1], partner))
    zc = []
    for d in sorted(range(1, NZ), key=lambda d: -min(d, NZ - d)):
        to = lax.rem(z + d, NZ)
        zc.append(go(remote(yq.at[pl.ds(2 * to, 2)], yr.at[pl.ds(2 * z, 2)], z_send.at[d], z_recv.at[d], zdev(d))))
    mine = pltpu.make_async_copy(yq.at[pl.ds(2 * z, 2)], yr.at[pl.ds(2 * z, 2)], z_recv.at[0])
    mine.start()

    cc.wait_recv()
    for i in range(NX):
        s1[i] = pk[c, i] + r0[i]
    xc = []
    for d in range(1, NX):
        to = lax.rem(x + d, NX)
        xc.append(go(remote(s1.at[to], r1.at[d - 1], x_send.at[d], x_recv.at[d], xdev(d))))
    ct.wait_recv()
    t1[...] = t0[...] + t0r[...]
    tx = [go(remote(t1, t1r.at[d - 1], t_send.at[d], t_recv.at[d], xdev(d))) for d in range(1, NX)]

    for cp in xc:
        cp.wait_recv()
    total = s1[x]
    for d in range(1, NX):
        total = total + r1[d - 1]
    s2[...] = total
    yc, yd = [], []
    for d in sorted(range(1, NY), key=lambda d: -min(d, NY - d)):
        to = lax.rem(y + d, NY)
        rows = pl.ds(pl.multiple_of(to * CH, CH), CH)
        yc.append(go(remote(s2.at[rows], r2.at[d - 1], y_send.at[d], y_recv.at[d], ydev(d))))
    for d in range(1, NY):
        yd.append(go(remote(s2.at[pl.ds(H, 8)], rd.at[d - 1], y_send.at[NY + d], y_recv.at[NY + d], ydev(d))))
    for cp in tx:
        cp.wait_recv()
    ttotal = t1[...]
    for d in range(1, NX):
        ttotal = ttotal + t1r[d - 1]
    t2[...] = ttotal
    ty = [go(remote(t2, t2r.at[d - 1], t_send.at[NX + d], t_recv.at[NX + d], ydev(d))) for d in range(1, NY)]

    for cp in yc:
        cp.wait_recv()
    total = s2[pl.ds(pl.multiple_of(y * CH, CH), CH), :]
    for d in range(1, NY):
        total = total + r2[d - 1]
    s3[...] = total
    own_rows = pl.ds(pl.multiple_of(y * CH, CH), CH)
    wc = []
    for d in sorted(range(1, NY), key=lambda d: -min(d, NY - d)):
        wc.append(go(remote(s3, gram.at[own_rows], w_send.at[d], w_recv.at[d], wdev(d))))
    for cp in yd:
        cp.wait_recv()
    total = s2[pl.ds(H, 8), :]
    for d in range(1, NY):
        total = total + rd[d - 1]
    sd[...] = total
    w0 = remote(s3, gram.at[own_rows], w_send.at[0], w_recv.at[0], wdev(0))
    w1 = remote(sd, gram.at[pl.ds(H, 8)], w_send.at[NY], w_recv.at[NY], wdev(0))
    l0 = pltpu.make_async_copy(s3, gram.at[own_rows], w_recv.at[0])
    l1 = pltpu.make_async_copy(sd, gram.at[pl.ds(H, 8)], w_recv.at[NY])

    @pl.when(k != z)
    def _():
        w0.start()
        w1.start()

    @pl.when(k == z)
    def _():
        l0.start()
        l1.start()

    for cp in ty:
        cp.wait_recv()
    ttotal = t2[...]
    for d in range(1, NY):
        ttotal = ttotal + t2r[d - 1]
    t2r[NY - 1] = ttotal
    count = jnp.int32(0)
    picked = [jnp.zeros((1, H), jnp.float32), jnp.zeros((1, H), jnp.float32)]
    for j in range(NB):
        same = jnp.where(owner_ref[0, j] == f, 1, 0)
        line = t2r[NY - 1, pl.ds(codes[j], 1), :]
        for s in range(2):
            weight = jnp.where(count == s, same, 0).astype(jnp.float32)
            picked[s] = picked[s] + line * weight
        count = count + same
    lane = lax.broadcasted_iota(jnp.int32, (1, 2), 1)
    sums = [jnp.sum(v, axis=1, keepdims=True) for v in picked]
    elements = H * H * NK * NY
    slot_ref[...] = jnp.sqrt(jnp.where(lane == 0, sums[0], sums[1]) / elements)

    for cp in wc:
        cp.wait_recv()
    l0.wait()
    l1.wait()
    a, b = newton_schulz(list(get_packed(gram)))
    put_packed(qall.at[k], a, b)

    xa = []
    b_own = go(remote(qall.at[k], qall.at[k], b_send.at[0], b_recv.at[0], partner))
    for d in range(1, NX):
        xa.append(go(remote(qall.at[k], qall.at[k], a_send.at[d], a_recv.at[d], xdev(d))))

    mine.wait()
    for cp in zc:
        cp.wait_recv()
    factor = step_size * 0.2 * math.sqrt(H * NK * NY)
    outs = []

    def apply(slot, i):
        for e, q in enumerate(get_packed(qall.at[slot])):
            high = q.astype(jnp.bfloat16)
            rest = (q - high.astype(jnp.float32)).astype(jnp.bfloat16)
            value = yr[2 * slot + e]
            ortho = jnp.dot(
                jnp.concatenate([high, rest], axis=1),
                jnp.concatenate([value, value], axis=0),
                preferred_element_type=jnp.float32,
            ).astype(jnp.bfloat16)
            outbuf[2 * slot + e] = (-factor * ortho.astype(jnp.float32)).astype(jnp.bfloat16)
        part = pl.ds(2 * slot, 2)
        st = pltpu.make_async_copy(outbuf.at[part], out_hbm.at[part], out_sem.at[i])
        st.start()
        outs.append(st)

    apply(k, 0)
    b_own.wait_recv()
    apply(2 * x + 1 - c, 1)
    fwd = []
    for d in range(1, NX):
        xa[d - 1].wait_recv()
        slot = 2 * lax.rem(x + NX - d, NX) + c
        fwd.append(go(remote(qall.at[slot], qall.at[slot], b_send.at[d], b_recv.at[d], partner)))
        apply(slot, 2 * d)
    for d in range(1, NX):
        fwd[d - 1].wait_recv()
        apply(2 * lax.rem(x + NX - d, NX) + 1 - c, 2 * d + 1)

    for st in outs + stores:
        st.wait()
    for cp in sent:
        cp.wait_send()

    @pl.when(k != z)
    def _():
        w0.wait_send()
        w1.wait_send()


def local(sizes, grads, momentum, owner_table, pool_map):
    NX, NY, NZ, NB = sizes
    NK = 2 * NX
    f32, bf16 = jnp.float32, jnp.bfloat16
    dma = pltpu.SemaphoreType.DMA
    hbm = pl.BlockSpec(memory_space=pl.ANY)
    scratch = [
        pltpu.VMEM((NB, H, H), bf16),
        pltpu.VMEM((NB, H, H), bf16),
        pltpu.VMEM((NB, H, H), bf16),
        pltpu.VMEM((NB, H, H), bf16),
        pltpu.VMEM((NB, H, H), bf16),
        pltpu.VMEM((NB, H, H), bf16),
        pltpu.VMEM((2, NX, PACKED, H), f32),
        pltpu.VMEM((NX, PACKED, H), f32),
        pltpu.VMEM((NX, PACKED, H), f32),
        pltpu.VMEM((NX - 1, PACKED, H), f32),
        pltpu.VMEM((PACKED, H), f32),
        pltpu.VMEM((NY - 1, H // NY, H), f32),
        pltpu.VMEM((NY - 1, 8, H), f32),
        pltpu.VMEM((H // NY, H), f32),
        pltpu.VMEM((8, H), f32),
        pltpu.VMEM((PACKED, H), f32),
        pltpu.VMEM((NK, PACKED, H), f32),
        pltpu.VMEM((NB, H, H), bf16),
        pltpu.VMEM((NB, H), f32),
        pltpu.VMEM((NB, H), f32),
        pltpu.VMEM((NB, H), f32),
        pltpu.VMEM((NX - 1, NB, H), f32),
        pltpu.VMEM((NB, H), f32),
        pltpu.VMEM((NY, NB, H), f32),
        dma((8,)),
        dma((4,)),
        dma((NK,)),
        dma((NZ,)),
        dma((NZ,)),
        dma((2,)),
        dma((2,)),
        dma((NX,)),
        dma((NX,)),
        dma((2 * NY,)),
        dma((2 * NY,)),
        dma((NX + NY,)),
        dma((NX + NY,)),
        dma((NY + 1,)),
        dma((NY + 1,)),
        dma((NX,)),
        dma((NX,)),
        dma((NX,)),
        dma((NX,)),
    ]
    smem = pl.BlockSpec(memory_space=pltpu.SMEM)
    return pl.pallas_call(
        functools.partial(kernel, sizes),
        out_shape=(
            jax.ShapeDtypeStruct(grads.shape, bf16),
            jax.ShapeDtypeStruct(grads.shape, bf16),
            jax.ShapeDtypeStruct((1, 2), f32),
        ),
        in_specs=[smem, smem, hbm, hbm],
        out_specs=(hbm, hbm, pl.BlockSpec(memory_space=pltpu.VMEM)),
        scratch_shapes=scratch,
        compiler_params=pltpu.CompilerParams(
            collective_id=0, has_side_effects=True
        ),
    )(owner_table.reshape(1, NB), pool_map, grads, momentum)


def solution(mesh, sizes=(4, 8, 8, 16)):
    in_specs = (P("tp", None, "fsdp"), P("tp", None, "fsdp"), P("tp", None), P("tp", None))
    out_specs = (P("tp", None, "fsdp"), P("tp", None, "fsdp"), P("tp", "fsdp"))
    return jax.shard_map(
        functools.partial(local, sizes), mesh=mesh, in_specs=in_specs, out_specs=out_specs, check_vma=False
    )
```

```python
import functools
import math

import jax
import jax.numpy as jnp
from jax import lax
from jax.experimental import pallas as pl
from jax.experimental.pallas import tpu as pltpu
from jax.sharding import PartitionSpec as P

ITERS = 3
momentum_rate = 0.95
step_size = 0.8
epsilon = 1e-07
poly_linear = 3.4445
poly_cubic = -4.775
poly_quintic = 2.0315

H = 128
PACKED = H + 8
MESH = pl.DeviceIdType.MESH


def masks():
    row = lax.broadcasted_iota(jnp.int32, (H, H), 0)
    col = lax.broadcasted_iota(jnp.int32, (H, H), 1)
    return row >= col, row == col


def put_packed(ref, a, b):
    low, diag = masks()
    ref[0:H, :] = jnp.where(low, a, b)
    last = jnp.sum(jnp.where(diag, b, 0.0), axis=0, keepdims=True)
    ref[H:PACKED, :] = jnp.broadcast_to(last, (8, H))


def get_packed(ref):
    low, diag = masks()
    both = ref[0:H, :]
    other = both.T
    last = jnp.broadcast_to(ref[H : H + 1, :], (H, H))
    a = jnp.where(low, both, other)
    b = jnp.where(diag, last, jnp.where(low, other, both))
    return a, b


def dot32(a, b):
    return jnp.dot(a, b, precision=lax.Precision.HIGHEST, preferred_element_type=jnp.float32)


def newton_schulz(grams):
    _, diag = masks()
    identity = jnp.where(diag, 1.0, 0.0)
    inverses, gs, qs = [], [], [None] * len(grams)
    for g in grams:
        squares = jnp.sum(jnp.where(diag, g, 0.0), keepdims=True)
        inverse = 1.0 / (jnp.sqrt(squares) + epsilon)
        inverses.append(inverse)
        gs.append(g * (inverse * inverse))
    for it in range(ITERS):
        g2 = [dot32(g, g) for g in gs]
        ms = [poly_linear * identity + poly_cubic * g + poly_quintic * s for g, s in zip(gs, g2)]
        if it < ITERS - 1:
            right = [dot32(g, m) for g, m in zip(gs, ms)]
        qs = [m if it == 0 else dot32(m, q) for m, q in zip(ms, qs)]
        if it < ITERS - 1:
            gs = [dot32(m, r) for m, r in zip(ms, right)]
    return [q * inverse for q, inverse in zip(qs, inverses)]


def kernel(
    sizes,
    owner_hbm,
    pool_hbm,
    g_hbm,
    m_hbm,
    nm_ref,
    out_ref,
    slot_ref,
    owner_ref,
    pool_ref,
    gbuf,
    mbuf,
    nes,
    yq,
    yr,
    pk,
    r0,
    s1,
    r1,
    s2,
    r2,
    rd,
    s3,
    sd,
    gram,
    qall,
    t0,
    t0r,
    t1,
    t1r,
    t2,
    t2r,
    in_sem,
    z_send,
    z_recv,
    c_send,
    c_recv,
    x_send,
    x_recv,
    y_send,
    y_recv,
    t_send,
    t_recv,
    w_send,
    w_recv,
    a_send,
    a_recv,
    b_send,
    b_recv,
):
    NX, NY, NZ, NB = sizes
    NK = 2 * NX
    CH = H // NY
    f = lax.axis_index("fsdp")
    z = lax.axis_index("tp")
    k = lax.rem(f, NK)
    y = lax.div(f, NK)
    x = lax.div(k, 2)
    c = lax.rem(k, 2)
    plane = lax.rem(k + NZ - z, NZ)

    def dev(yy, xx, cc, zz):
        return ((yy * NX + xx) * 2 + cc, zz)

    partner = dev(y, x, 1 - c, z)

    def xdev(d):
        return dev(y, lax.rem(x + d, NX), c, z)

    def ydev(d):
        return dev(lax.rem(y + d, NY), x, c, z)

    def zdev(d):
        return dev(y, x, c, lax.rem(z + d, NZ))

    def wdev(d):
        return (lax.rem(y + d, NY) * NK + k, plane)

    def remote(src, dst, send, recv, device):
        return pltpu.make_async_remote_copy(
            src_ref=src, dst_ref=dst, send_sem=send, recv_sem=recv, device_id=device, device_id_type=MESH
        )

    own_copy = pltpu.make_async_copy(owner_hbm, owner_ref, in_sem.at[8])
    pool_copy = pltpu.make_async_copy(pool_hbm, pool_ref, in_sem.at[9])
    own_copy.start()
    pool_copy.start()
    CHUNKS = 4
    per = NB // CHUNKS
    loads = []
    for i in range(CHUNKS):
        part = pl.ds(i * per, per)
        lg = pltpu.make_async_copy(g_hbm.at[part], gbuf.at[part], in_sem.at[2 * i])
        lm = pltpu.make_async_copy(m_hbm.at[part], mbuf.at[part], in_sem.at[2 * i + 1])
        lg.start()
        lm.start()
        loads.append((lg, lm))

    barrier = pltpu.get_barrier_semaphore()

    def greet(device):
        pl.semaphore_signal(barrier, inc=1, device_id=device, device_id_type=MESH)

    for d in range(1, NZ):
        greet(zdev(d))
    for d in range(1, NY):
        greet(ydev(d))
    for d in range(1, NX):
        greet(xdev(d))
    greet(partner)

    own_copy.wait()
    pool_copy.wait()
    codes = [pool_ref[0, j] for j in range(NB)]
    source = []
    for q in range(NB):
        at = jnp.int32(0)
        for j in range(1, NB):
            at = jnp.where(codes[j] == q, j, at)
        source.append(at)

    for i in range(CHUNKS):
        for cp in loads[i]:
            cp.wait()
        for j in range(i * per, (i + 1) * per):
            grad = gbuf[j].astype(jnp.float32)
            velocity = momentum_rate * mbuf[j].astype(jnp.float32) + grad
            nm_ref[j] = velocity.astype(jnp.bfloat16)
            nes[j] = (grad + momentum_rate * velocity).astype(jnp.bfloat16)

    for p in range(NZ):
        grams = []
        for e in range(2):
            q = 2 * p + e
            value = nes[source[q]]
            yq[q] = value
            wide = value.astype(jnp.float32)
            t0[q : q + 1, :] = jnp.sum(wide * wide, axis=0, keepdims=True)
            grams.append(
                lax.dot_general(value, value, (((1,), (1,)), ((), ())), preferred_element_type=jnp.float32)
            )
        place = lax.rem(p + z, NK)
        put_packed(pk.at[lax.rem(place, 2), lax.div(place, 2)], *grams)

    pl.semaphore_wait(barrier, (NZ - 1) + (NY - 1) + (NX - 1) + 1 )

    sent = []

    def go(copy):
        copy.start()
        sent.append(copy)
        return copy

    cc = go(remote(pk.at[1 - c], r0, c_send.at[0], c_recv.at[0], partner))
    ct = go(remote(t0, t0r, c_send.at[1], c_recv.at[1], partner))
    zc = []
    for d in sorted(range(1, NZ), key=lambda d: -min(d, NZ - d)):
        to = lax.rem(z + d, NZ)
        zc.append(go(remote(yq.at[pl.ds(2 * to, 2)], yr.at[pl.ds(2 * z, 2)], z_send.at[d], z_recv.at[d], zdev(d))))
    mine = pltpu.make_async_copy(yq.at[pl.ds(2 * z, 2)], yr.at[pl.ds(2 * z, 2)], z_recv.at[0])
    mine.start()

    cc.wait_recv()
    for i in range(NX):
        s1[i] = pk[c, i] + r0[i]
    xc = []
    for d in range(1, NX):
        to = lax.rem(x + d, NX)
        xc.append(go(remote(s1.at[to], r1.at[d - 1], x_send.at[d], x_recv.at[d], xdev(d))))
    ct.wait_recv()
    t1[...] = t0[...] + t0r[...]
    tx = [go(remote(t1, t1r.at[d - 1], t_send.at[d], t_recv.at[d], xdev(d))) for d in range(1, NX)]

    for cp in xc:
        cp.wait_recv()
    total = s1[x]
    for d in range(1, NX):
        total = total + r1[d - 1]
    s2[...] = total
    yc, yd = [], []
    for d in sorted(range(1, NY), key=lambda d: -min(d, NY - d)):
        to = lax.rem(y + d, NY)
        rows = pl.ds(pl.multiple_of(to * CH, CH), CH)
        yc.append(go(remote(s2.at[rows], r2.at[d - 1], y_send.at[d], y_recv.at[d], ydev(d))))
    for d in range(1, NY):
        yd.append(go(remote(s2.at[pl.ds(H, 8)], rd.at[d - 1], y_send.at[NY + d], y_recv.at[NY + d], ydev(d))))
    for cp in tx:
        cp.wait_recv()
    ttotal = t1[...]
    for d in range(1, NX):
        ttotal = ttotal + t1r[d - 1]
    t2[...] = ttotal
    ty = [go(remote(t2, t2r.at[d - 1], t_send.at[NX + d], t_recv.at[NX + d], ydev(d))) for d in range(1, NY)]

    for cp in yc:
        cp.wait_recv()
    total = s2[pl.ds(pl.multiple_of(y * CH, CH), CH), :]
    for d in range(1, NY):
        total = total + r2[d - 1]
    s3[...] = total
    own_rows = pl.ds(pl.multiple_of(y * CH, CH), CH)
    wc = []
    for d in sorted(range(1, NY), key=lambda d: -min(d, NY - d)):
        wc.append(go(remote(s3, gram.at[own_rows], w_send.at[d], w_recv.at[d], wdev(d))))
    for cp in yd:
        cp.wait_recv()
    total = s2[pl.ds(H, 8), :]
    for d in range(1, NY):
        total = total + rd[d - 1]
    sd[...] = total
    w0 = remote(s3, gram.at[own_rows], w_send.at[0], w_recv.at[0], wdev(0))
    w1 = remote(sd, gram.at[pl.ds(H, 8)], w_send.at[NY], w_recv.at[NY], wdev(0))
    l0 = pltpu.make_async_copy(s3, gram.at[own_rows], w_recv.at[0])
    l1 = pltpu.make_async_copy(sd, gram.at[pl.ds(H, 8)], w_recv.at[NY])

    @pl.when(plane != z)
    def _():
        w0.start()
        w1.start()

    @pl.when(plane == z)
    def _():
        l0.start()
        l1.start()

    for cp in ty:
        cp.wait_recv()
    ttotal = t2[...]
    for d in range(1, NY):
        ttotal = ttotal + t2r[d - 1]
    t2r[NY - 1] = ttotal
    count = jnp.int32(0)
    picked = [jnp.zeros((1, H), jnp.float32), jnp.zeros((1, H), jnp.float32)]
    for j in range(NB):
        same = jnp.where(owner_ref[0, j] == f, 1, 0)
        line = t2r[NY - 1, pl.ds(codes[j], 1), :]
        for s in range(2):
            weight = jnp.where(count == s, same, 0).astype(jnp.float32)
            picked[s] = picked[s] + line * weight
        count = count + same
    lane = lax.broadcasted_iota(jnp.int32, (1, 2), 1)
    sums = [jnp.sum(v, axis=1, keepdims=True) for v in picked]
    elements = H * H * NK * NY
    slot_ref[...] = jnp.sqrt(jnp.where(lane == 0, sums[0], sums[1]) / elements)

    for cp in wc:
        cp.wait_recv()
    l0.wait()
    l1.wait()
    a, b = newton_schulz(list(get_packed(gram)))
    put_packed(qall.at[k], a, b)

    xa = []
    b_own = go(remote(qall.at[k], qall.at[k], b_send.at[0], b_recv.at[0], partner))
    for d in range(1, NX):
        xa.append(go(remote(qall.at[k], qall.at[k], a_send.at[d], a_recv.at[d], xdev(d))))

    mine.wait()
    for cp in zc:
        cp.wait_recv()
    factor = step_size * 0.2 * math.sqrt(H * NK * NY)

    def apply(at):
        slot = lax.rem(at + NZ - z, NZ)
        for e, q in enumerate(get_packed(qall.at[at])):
            high = q.astype(jnp.bfloat16)
            rest = (q - high.astype(jnp.float32)).astype(jnp.bfloat16)
            value = yr[2 * slot + e]
            ortho = jnp.dot(
                jnp.concatenate([high, rest], axis=1),
                jnp.concatenate([value, value], axis=0),
                preferred_element_type=jnp.float32,
            ).astype(jnp.bfloat16)
            out_ref[2 * slot + e] = (-factor * ortho.astype(jnp.float32)).astype(jnp.bfloat16)

    apply(k)
    b_own.wait_recv()
    apply(2 * x + 1 - c)
    fwd = []
    for d in range(1, NX):
        xa[d - 1].wait_recv()
        slot = 2 * lax.rem(x + NX - d, NX) + c
        fwd.append(go(remote(qall.at[slot], qall.at[slot], b_send.at[d], b_recv.at[d], partner)))
        apply(slot)
    for d in range(1, NX):
        fwd[d - 1].wait_recv()
        apply(2 * lax.rem(x + NX - d, NX) + 1 - c)

    for cp in sent:
        cp.wait_send()

    @pl.when(plane != z)
    def _():
        w0.wait_send()
        w1.wait_send()


def local(sizes, grads, momentum, owner_table, pool_map):
    NX, NY, NZ, NB = sizes
    NK = 2 * NX
    f32, bf16 = jnp.float32, jnp.bfloat16
    dma = pltpu.SemaphoreType.DMA
    hbm = pl.BlockSpec(memory_space=pltpu.HBM)
    scratch = [
        pltpu.SMEM((1, NB), jnp.int32),
        pltpu.SMEM((1, NB), jnp.int32),
        pltpu.VMEM((NB, H, H), bf16),
        pltpu.VMEM((NB, H, H), bf16),
        pltpu.VMEM((NB, H, H), bf16),
        pltpu.VMEM((NB, H, H), bf16),
        pltpu.VMEM((NB, H, H), bf16),
        pltpu.VMEM((2, NX, PACKED, H), f32),
        pltpu.VMEM((NX, PACKED, H), f32),
        pltpu.VMEM((NX, PACKED, H), f32),
        pltpu.VMEM((NX - 1, PACKED, H), f32),
        pltpu.VMEM((PACKED, H), f32),
        pltpu.VMEM((NY - 1, H // NY, H), f32),
        pltpu.VMEM((NY - 1, 8, H), f32),
        pltpu.VMEM((H // NY, H), f32),
        pltpu.VMEM((8, H), f32),
        pltpu.VMEM((PACKED, H), f32),
        pltpu.VMEM((NK, PACKED, H), f32),
        pltpu.VMEM((NB, H), f32),
        pltpu.VMEM((NB, H), f32),
        pltpu.VMEM((NB, H), f32),
        pltpu.VMEM((NX - 1, NB, H), f32),
        pltpu.VMEM((NB, H), f32),
        pltpu.VMEM((NY, NB, H), f32),
        dma((10,)),
        dma((NZ,)),
        dma((NZ,)),
        dma((2,)),
        dma((2,)),
        dma((NX,)),
        dma((NX,)),
        dma((2 * NY,)),
        dma((2 * NY,)),
        dma((NX + NY,)),
        dma((NX + NY,)),
        dma((NY + 1,)),
        dma((NY + 1,)),
        dma((NX,)),
        dma((NX,)),
        dma((NX,)),
        dma((NX,)),
    ]
    return pl.pallas_call(
        functools.partial(kernel, sizes),
        out_shape=(
            jax.ShapeDtypeStruct(grads.shape, bf16),
            jax.ShapeDtypeStruct(grads.shape, bf16),
            jax.ShapeDtypeStruct((1, 2), f32),
        ),
        in_specs=[hbm] * 4,
        out_specs=(pl.BlockSpec(memory_space=pltpu.VMEM),) * 3,
        scratch_shapes=scratch,
        compiler_params=pltpu.CompilerParams(
            collective_id=0, has_side_effects=True, vmem_limit_bytes=24 * 1024 * 1024
        ),
    )(
        *(
            pltpu.with_memory_space_constraint(v, pltpu.HBM)
            for v in (owner_table.reshape(1, NB), pool_map, grads, momentum)
        )
    )


def solution(mesh, sizes=(4, 8, 8, 16)):
    in_specs = (P("tp", None, "fsdp"), P("tp", None, "fsdp"), P("tp", None), P("tp", None))
    out_specs = (P("tp", None, "fsdp"), P("tp", None, "fsdp"), P("tp", "fsdp"))
    return jax.shard_map(
        functools.partial(local, sizes), mesh=mesh, in_specs=in_specs, out_specs=out_specs, check_vma=False
    )
```

```python
import functools
import math

import jax
import jax.numpy as jnp
from jax import lax
from jax.experimental import pallas as pl
from jax.experimental.pallas import tpu as pltpu
from jax.sharding import PartitionSpec as P

ITERS = 3
momentum_rate = 0.95
step_size = 0.8
epsilon = 1e-07
poly_linear = 3.4445
poly_cubic = -4.775
poly_quintic = 2.0315

H = 128
PACKED = H + 8
MESH = pl.DeviceIdType.MESH


def masks():
    row = lax.broadcasted_iota(jnp.int32, (H, H), 0)
    col = lax.broadcasted_iota(jnp.int32, (H, H), 1)
    return row >= col, row == col


def put_packed(ref, a, b):
    low, diag = masks()
    ref[0:H, :] = jnp.where(low, a, b)
    last = jnp.sum(jnp.where(diag, b, 0.0), axis=0, keepdims=True)
    ref[H:PACKED, :] = jnp.broadcast_to(last, (8, H))


def get_packed(ref):
    low, diag = masks()
    both = ref[0:H, :]
    other = both.T
    last = jnp.broadcast_to(ref[H : H + 1, :], (H, H))
    a = jnp.where(low, both, other)
    b = jnp.where(diag, last, jnp.where(low, other, both))
    return a, b


def dot32(a, b):
    return jnp.dot(a, b, precision=lax.Precision.HIGHEST, preferred_element_type=jnp.float32)


def newton_schulz(grams):
    _, diag = masks()
    identity = jnp.where(diag, 1.0, 0.0)
    inverses, gs, qs = [], [], [None] * len(grams)
    for g in grams:
        squares = jnp.sum(jnp.where(diag, g, 0.0), keepdims=True)
        inverse = 1.0 / (jnp.sqrt(squares) + epsilon)
        inverses.append(inverse)
        gs.append(g * (inverse * inverse))
    for it in range(ITERS):
        g2 = [dot32(g, g) for g in gs]
        ms = [poly_linear * identity + poly_cubic * g + poly_quintic * s for g, s in zip(gs, g2)]
        if it < ITERS - 1:
            right = [dot32(g, m) for g, m in zip(gs, ms)]
        qs = [m if it == 0 else dot32(m, q) for m, q in zip(ms, qs)]
        if it < ITERS - 1:
            gs = [dot32(m, r) for m, r in zip(ms, right)]
    return [q * inverse for q, inverse in zip(qs, inverses)]


def kernel(
    sizes,
    owner_hbm,
    pool_hbm,
    g_hbm,
    m_hbm,
    nm_ref,
    out_ref,
    slot_ref,
    owner_ref,
    pool_ref,
    gbuf,
    mbuf,
    yq,
    yr,
    pk,
    r0,
    s1,
    r1,
    s2,
    r2,
    rd,
    s3,
    sd,
    gram,
    qall,
    t0,
    t0r,
    t1,
    t1r,
    t2,
    t2r,
    in_sem,
    z_send,
    z_recv,
    c_send,
    c_recv,
    x_send,
    x_recv,
    y_send,
    y_recv,
    t_send,
    t_recv,
    w_send,
    w_recv,
    a_send,
    a_recv,
    b_send,
    b_recv,
):
    NX, NY, NZ, NB = sizes
    NK = 2 * NX
    CH = H // NY
    f = lax.axis_index("fsdp")
    z = lax.axis_index("tp")
    k = lax.rem(f, NK)
    y = lax.div(f, NK)
    x = lax.div(k, 2)
    c = lax.rem(k, 2)
    plane = lax.rem(k + NZ - z, NZ)

    def dev(yy, xx, cc, zz):
        return ((yy * NX + xx) * 2 + cc, zz)

    partner = dev(y, x, 1 - c, z)

    def xdev(d):
        return dev(y, lax.rem(x + d, NX), c, z)

    def ydev(d):
        return dev(lax.rem(y + d, NY), x, c, z)

    def zdev(d):
        return dev(y, x, c, lax.rem(z + d, NZ))

    def wdev(d):
        return (lax.rem(y + d, NY) * NK + k, plane)

    def remote(src, dst, send, recv, device):
        return pltpu.make_async_remote_copy(
            src_ref=src, dst_ref=dst, send_sem=send, recv_sem=recv, device_id=device, device_id_type=MESH
        )

    own_copy = pltpu.make_async_copy(owner_hbm, owner_ref, in_sem.at[8])
    pool_copy = pltpu.make_async_copy(pool_hbm, pool_ref, in_sem.at[9])
    own_copy.start()
    pool_copy.start()
    CHUNKS = 4
    per = NB // CHUNKS
    loads = []
    for i in range(CHUNKS):
        part = pl.ds(i * per, per)
        lg = pltpu.make_async_copy(g_hbm.at[part], gbuf.at[part], in_sem.at[2 * i])
        lm = pltpu.make_async_copy(m_hbm.at[part], mbuf.at[part], in_sem.at[2 * i + 1])
        lg.start()
        lm.start()
        loads.append((lg, lm))

    barrier = pltpu.get_barrier_semaphore()

    def greet(device):
        pl.semaphore_signal(barrier, inc=1, device_id=device, device_id_type=MESH)

    for d in range(1, NZ):
        greet(zdev(d))
    for d in range(1, NY):
        greet(ydev(d))
    for d in range(1, NX):
        greet(xdev(d))
    greet(partner)

    own_copy.wait()
    pool_copy.wait()
    codes = [pool_ref[0, j] for j in range(NB)]

    def source(q):
        at = jnp.int32(0)
        for j in range(1, NB):
            at = jnp.where(codes[j] == q, j, at)
        return at

    for pair in loads:
        for cp in pair:
            cp.wait()

    def nesterov(j):
        grad = gbuf[j].astype(jnp.float32)
        velocity = momentum_rate * mbuf[j].astype(jnp.float32) + grad
        return velocity, (grad + momentum_rate * velocity).astype(jnp.bfloat16)

    def make_pair(core, at):
        p = lax.rem(2 * at + core + NZ - z, NZ)
        grams = []
        for e in range(2):
            q = 2 * p + e
            _, value = nesterov(source(q))
            yq[q] = value
            wide = value.astype(jnp.float32)
            t0[pl.ds(q, 1), :] = jnp.sum(wide * wide, axis=0, keepdims=True)
            grams.append(
                lax.dot_general(value, value, (((1,), (1,)), ((), ())), preferred_element_type=jnp.float32)
            )
        put_packed(pk.at[core, at], *grams)

    sent = []

    def go(copy):
        copy.start()
        sent.append(copy)
        return copy

    left, right, far = lax.rem(x + NX - 1, NX), lax.rem(x + 1, NX), lax.rem(x + 2, NX)
    order = [far, left, right, x]
    cc = []
    for i, at in enumerate(order):
        make_pair(1 - c, at)
        if i == 0:
            pl.semaphore_wait(barrier, (NZ - 1) + (NY - 1) + (NX - 1) + 1)
        cc.append(go(remote(pk.at[1 - c, at], r0.at[at], c_send.at[i], c_recv.at[i], partner)))
    for at in order:
        make_pair(c, at)
    ct = go(remote(t0, t0r, c_send.at[NX], c_recv.at[NX], partner))

    upper, lower = pl.ds(0, H // 2), pl.ds(H // 2, PACKED - H // 2)
    to_right = {"device": dev(y, right, c, z)}
    to_left = {"device": dev(y, left, c, z)}
    cc[0].wait_recv()
    s1[far] = pk[c, far] + r0[far]
    f_up = go(remote(s1.at[far, upper], r1.at[0, upper], x_send.at[0], x_recv.at[0], **to_right))
    f_low = go(remote(s1.at[far, lower], r1.at[0, lower], x_send.at[1], x_recv.at[1], **to_left))
    cc[1].wait_recv()
    s1[left] = pk[c, left] + r0[left]
    d_up = go(remote(s1.at[left, upper], r1.at[1, upper], x_send.at[2], x_recv.at[2], **to_left))
    cc[2].wait_recv()
    s1[right] = pk[c, right] + r0[right]
    d_low = go(remote(s1.at[right, lower], r1.at[1, lower], x_send.at[3], x_recv.at[3], **to_right))
    ct.wait_recv()
    t1[...] = t0[...] + t0r[...]
    tx = [go(remote(t1, t1r.at[d - 1], t_send.at[d], t_recv.at[d], xdev(d))) for d in range(1, NX)]
    cc[3].wait_recv()
    s1[x] = pk[c, x] + r0[x]
    f_up.wait_recv()
    r0[0, upper, :] = s1[right, upper, :] + r1[0, upper, :]
    g_up = go(remote(r0.at[0, upper], r1.at[2, upper], x_send.at[4], x_recv.at[4], **to_right))
    f_low.wait_recv()
    r0[0, lower, :] = s1[left, lower, :] + r1[0, lower, :]
    g_low = go(remote(r0.at[0, lower], r1.at[2, lower], x_send.at[5], x_recv.at[5], **to_left))

    zc = []
    for d in sorted(range(1, NZ), key=lambda d: -min(d, NZ - d)):
        to = lax.rem(z + d, NZ)
        zc.append(go(remote(yq.at[pl.ds(2 * to, 2)], yr.at[pl.ds(2 * z, 2)], z_send.at[d], z_recv.at[d], zdev(d))))
    mine = pltpu.make_async_copy(yq.at[pl.ds(2 * z, 2)], yr.at[pl.ds(2 * z, 2)], z_recv.at[0])
    mine.start()

    for j in range(NB):
        nm_ref[j] = nesterov(j)[0].astype(jnp.bfloat16)

    for cp in (d_up, d_low, g_up, g_low):
        cp.wait_recv()
    s2[...] = s1[x] + r1[1] + r1[2]
    yc, yd = [], []
    for d in sorted(range(1, NY), key=lambda d: -min(d, NY - d)):
        to = lax.rem(y + d, NY)
        rows = pl.ds(pl.multiple_of(to * CH, CH), CH)
        yc.append(go(remote(s2.at[rows], r2.at[d - 1], y_send.at[d], y_recv.at[d], ydev(d))))
    for d in range(1, NY):
        yd.append(go(remote(s2.at[pl.ds(H, 8)], rd.at[d - 1], y_send.at[NY + d], y_recv.at[NY + d], ydev(d))))
    for cp in tx:
        cp.wait_recv()
    ttotal = t1[...]
    for d in range(1, NX):
        ttotal = ttotal + t1r[d - 1]
    t2[...] = ttotal
    ty = [go(remote(t2, t2r.at[d - 1], t_send.at[NX + d], t_recv.at[NX + d], ydev(d))) for d in range(1, NY)]

    for cp in yc:
        cp.wait_recv()
    total = s2[pl.ds(pl.multiple_of(y * CH, CH), CH), :]
    for d in range(1, NY):
        total = total + r2[d - 1]
    s3[...] = total
    own_rows = pl.ds(pl.multiple_of(y * CH, CH), CH)
    wc = []
    for d in sorted(range(1, NY), key=lambda d: -min(d, NY - d)):
        wc.append(go(remote(s3, gram.at[own_rows], w_send.at[d], w_recv.at[d], wdev(d))))
    for cp in yd:
        cp.wait_recv()
    total = s2[pl.ds(H, 8), :]
    for d in range(1, NY):
        total = total + rd[d - 1]
    sd[...] = total
    w0 = remote(s3, gram.at[own_rows], w_send.at[0], w_recv.at[0], wdev(0))
    w1 = remote(sd, gram.at[pl.ds(H, 8)], w_send.at[NY], w_recv.at[NY], wdev(0))
    l0 = pltpu.make_async_copy(s3, gram.at[own_rows], w_recv.at[0])
    l1 = pltpu.make_async_copy(sd, gram.at[pl.ds(H, 8)], w_recv.at[NY])

    @pl.when(plane != z)
    def _():
        w0.start()
        w1.start()

    @pl.when(plane == z)
    def _():
        l0.start()
        l1.start()

    for cp in ty:
        cp.wait_recv()
    ttotal = t2[...]
    for d in range(1, NY):
        ttotal = ttotal + t2r[d - 1]
    t2r[NY - 1] = ttotal
    count = jnp.int32(0)
    picked = [jnp.zeros((1, H), jnp.float32), jnp.zeros((1, H), jnp.float32)]
    for j in range(NB):
        same = jnp.where(owner_ref[0, j] == f, 1, 0)
        line = t2r[NY - 1, pl.ds(codes[j], 1), :]
        for s in range(2):
            weight = jnp.where(count == s, same, 0).astype(jnp.float32)
            picked[s] = picked[s] + line * weight
        count = count + same
    lane = lax.broadcasted_iota(jnp.int32, (1, 2), 1)
    sums = [jnp.sum(v, axis=1, keepdims=True) for v in picked]
    elements = H * H * NK * NY
    slot_ref[...] = jnp.sqrt(jnp.where(lane == 0, sums[0], sums[1]) / elements)

    for cp in wc:
        cp.wait_recv()
    l0.wait()
    l1.wait()
    a, b = newton_schulz(list(get_packed(gram)))
    put_packed(qall.at[k], a, b)

    b_own = go(remote(qall.at[k], qall.at[k], b_send.at[0], b_recv.at[0], partner))

    def pass_on(at, rows, i, device):
        return go(remote(qall.at[at, rows], qall.at[at, rows], a_send.at[i], a_recv.at[i], device))

    k_left, k_right, k_far = 2 * left + c, 2 * right + c, 2 * far + c
    up_right = pass_on(k, upper, 0, to_right["device"])
    low_left = pass_on(k, lower, 1, to_left["device"])
    low_right = pass_on(k, lower, 2, to_right["device"])
    up_left = pass_on(k, upper, 3, to_left["device"])

    mine.wait()
    for cp in zc:
        cp.wait_recv()
    factor = step_size * 0.2 * math.sqrt(H * NK * NY)

    def apply(at):
        slot = lax.rem(at + NZ - z, NZ)
        for e, q in enumerate(get_packed(qall.at[at])):
            high = q.astype(jnp.bfloat16)
            rest = (q - high.astype(jnp.float32)).astype(jnp.bfloat16)
            value = yr[2 * slot + e]
            ortho = jnp.dot(
                jnp.concatenate([high, rest], axis=1),
                jnp.concatenate([value, value], axis=0),
                preferred_element_type=jnp.float32,
            ).astype(jnp.bfloat16)
            out_ref[2 * slot + e] = (-factor * ortho.astype(jnp.float32)).astype(jnp.bfloat16)

    def across(at, i):
        return go(remote(qall.at[at], qall.at[at], b_send.at[i], b_recv.at[i], partner))

    apply(k)
    up_right.wait_recv()
    far_up = pass_on(k_left, upper, 4, to_right["device"])
    low_left.wait_recv()
    far_low = pass_on(k_right, lower, 5, to_left["device"])
    b_own.wait_recv()
    apply(2 * x + 1 - c)
    low_right.wait_recv()
    b_left = across(k_left, 1)
    up_left.wait_recv()
    b_right = across(k_right, 2)
    apply(k_left)
    apply(k_right)
    far_up.wait_recv()
    far_low.wait_recv()
    b_far = across(k_far, 3)
    b_left.wait_recv()
    apply(2 * left + 1 - c)
    b_right.wait_recv()
    apply(2 * right + 1 - c)
    apply(k_far)
    b_far.wait_recv()
    apply(2 * far + 1 - c)

    for cp in sent:
        cp.wait_send()

    @pl.when(plane != z)
    def _():
        w0.wait_send()
        w1.wait_send()


def writer(*refs):
    copies = [pltpu.make_async_copy(refs[i], refs[3 + i], refs[6].at[i]) for i in range(3)]
    for cp in copies:
        cp.start()
    for cp in copies:
        cp.wait()


def written(results):
    vmem = pl.BlockSpec(memory_space=pltpu.VMEM)
    return pl.pallas_call(
        writer,
        out_shape=tuple(jax.ShapeDtypeStruct(v.shape, v.dtype) for v in results),
        in_specs=[vmem] * 3,
        out_specs=(pl.BlockSpec(memory_space=pltpu.HBM),) * 3,
        scratch_shapes=[pltpu.SemaphoreType.DMA((3,))],
        compiler_params=pltpu.CompilerParams(vmem_limit_bytes=8 * 1024 * 1024),
    )(*results)


def local(sizes, grads, momentum, owner_table, pool_map):
    NX, NY, NZ, NB = sizes
    NK = 2 * NX
    f32, bf16 = jnp.float32, jnp.bfloat16
    dma = pltpu.SemaphoreType.DMA
    hbm = pl.BlockSpec(memory_space=pltpu.HBM)
    scratch = [
        pltpu.SMEM((1, NB), jnp.int32),
        pltpu.SMEM((1, NB), jnp.int32),
        pltpu.VMEM((NB, H, H), bf16),
        pltpu.VMEM((NB, H, H), bf16),
        pltpu.VMEM((NB, H, H), bf16),
        pltpu.VMEM((NB, H, H), bf16),
        pltpu.VMEM((2, NX, PACKED, H), f32),
        pltpu.VMEM((NX, PACKED, H), f32),
        pltpu.VMEM((NX, PACKED, H), f32),
        pltpu.VMEM((NX - 1, PACKED, H), f32),
        pltpu.VMEM((PACKED, H), f32),
        pltpu.VMEM((NY - 1, H // NY, H), f32),
        pltpu.VMEM((NY - 1, 8, H), f32),
        pltpu.VMEM((H // NY, H), f32),
        pltpu.VMEM((8, H), f32),
        pltpu.VMEM((PACKED, H), f32),
        pltpu.VMEM((NK, PACKED, H), f32),
        pltpu.VMEM((NB, H), f32),
        pltpu.VMEM((NB, H), f32),
        pltpu.VMEM((NB, H), f32),
        pltpu.VMEM((NX - 1, NB, H), f32),
        pltpu.VMEM((NB, H), f32),
        pltpu.VMEM((NY, NB, H), f32),
        dma((10,)),
        dma((NZ,)),
        dma((NZ,)),
        dma((NX + 1,)),
        dma((NX + 1,)),
        dma((6,)),
        dma((6,)),
        dma((2 * NY,)),
        dma((2 * NY,)),
        dma((NX + NY,)),
        dma((NX + NY,)),
        dma((NY + 1,)),
        dma((NY + 1,)),
        dma((6,)),
        dma((6,)),
        dma((NX,)),
        dma((NX,)),
    ]
    results = pl.pallas_call(
        functools.partial(kernel, sizes),
        out_shape=(
            jax.ShapeDtypeStruct(grads.shape, bf16),
            jax.ShapeDtypeStruct(grads.shape, bf16),
            jax.ShapeDtypeStruct((1, 2), f32),
        ),
        in_specs=[hbm] * 4,
        out_specs=(pl.BlockSpec(memory_space=pltpu.VMEM),) * 3,
        scratch_shapes=scratch,
        compiler_params=pltpu.CompilerParams(
            collective_id=0, has_side_effects=True, vmem_limit_bytes=24 * 1024 * 1024
        ),
    )(
        *(
            pltpu.with_memory_space_constraint(v, pltpu.HBM)
            for v in (owner_table.reshape(1, NB), pool_map, grads, momentum)
        )
    )
    return written(results)


def solution(mesh, sizes=(4, 8, 8, 16)):
    in_specs = (P("tp", None, "fsdp"), P("tp", None, "fsdp"), P("tp", None), P("tp", None))
    out_specs = (P("tp", None, "fsdp"), P("tp", None, "fsdp"), P("tp", "fsdp"))
    return jax.shard_map(
        functools.partial(local, sizes), mesh=mesh, in_specs=in_specs, out_specs=out_specs, check_vma=False
    )
```

```python
import functools
import math

import jax
import jax.numpy as jnp
from jax import lax
from jax.experimental import pallas as pl
from jax.experimental.pallas import tpu as pltpu
from jax.sharding import PartitionSpec as P

ITERS = 3
momentum_rate = 0.95
step_size = 0.8
epsilon = 1e-07
poly_linear = 3.4445
poly_cubic = -4.775
poly_quintic = 2.0315

H = 128
PACKED = H + 8
MESH = pl.DeviceIdType.MESH


def masks():
    row = lax.broadcasted_iota(jnp.int32, (H, H), 0)
    col = lax.broadcasted_iota(jnp.int32, (H, H), 1)
    return row >= col, row == col


def put_packed(ref, a, b):
    low, diag = masks()
    ref[0:H, :] = jnp.where(low, a, b)
    last = jnp.sum(jnp.where(diag, b, 0.0), axis=0, keepdims=True)
    ref[H:PACKED, :] = jnp.broadcast_to(last, (8, H))


def get_packed(ref):
    low, diag = masks()
    both = ref[0:H, :]
    other = both.T
    last = jnp.broadcast_to(ref[H : H + 1, :], (H, H))
    a = jnp.where(low, both, other)
    b = jnp.where(diag, last, jnp.where(low, other, both))
    return a, b


def dot32(a, b):
    return jnp.dot(a, b, precision=lax.Precision.HIGHEST, preferred_element_type=jnp.float32)


def newton_schulz(grams):
    _, diag = masks()
    identity = jnp.where(diag, 1.0, 0.0)
    inverses, gs, qs = [], [], [None] * len(grams)
    for g in grams:
        squares = jnp.sum(jnp.where(diag, g, 0.0), keepdims=True)
        inverse = 1.0 / (jnp.sqrt(squares) + epsilon)
        inverses.append(inverse)
        gs.append(g * (inverse * inverse))
    for it in range(ITERS):
        g2 = [dot32(g, g) for g in gs]
        ms = [poly_linear * identity + poly_cubic * g + poly_quintic * s for g, s in zip(gs, g2)]
        if it < ITERS - 1:
            right = [dot32(g, m) for g, m in zip(gs, ms)]
        qs = [m if it == 0 else dot32(m, q) for m, q in zip(ms, qs)]
        if it < ITERS - 1:
            gs = [dot32(m, r) for m, r in zip(ms, right)]
    return [q * inverse for q, inverse in zip(qs, inverses)]


def kernel(
    sizes,
    owner_hbm,
    pool_hbm,
    g_hbm,
    m_hbm,
    nm_ref,
    out_ref,
    slot_ref,
    owner_ref,
    pool_ref,
    gbuf,
    mbuf,
    yq,
    yr,
    pk,
    r0,
    s1,
    r1,
    s2,
    r2,
    rd,
    s3,
    sd,
    gram,
    qall,
    t0,
    t0r,
    t1,
    t1r,
    t2,
    t2r,
    in_sem,
    z_send,
    z_recv,
    c_send,
    c_recv,
    x_send,
    x_recv,
    y_send,
    y_recv,
    t_send,
    t_recv,
    w_send,
    w_recv,
    a_send,
    a_recv,
    b_send,
    b_recv,
):
    NX, NY, NZ, NB = sizes
    NK = 2 * NX
    CH = H // NY
    f = lax.axis_index("fsdp")
    z = lax.axis_index("tp")
    k = lax.rem(f, NK)
    y = lax.div(f, NK)
    x = lax.div(k, 2)
    c = lax.rem(k, 2)
    plane = lax.rem(k + NZ - z, NZ)
    k_far = lax.rem(k + NX, NK)

    def dev(yy, xx, cc, zz):
        return ((yy * NX + xx) * 2 + cc, zz)

    partner = dev(y, x, 1 - c, z)

    def xdev(d):
        return dev(y, lax.rem(x + d, NX), c, z)

    def ydev(d):
        return dev(lax.rem(y + d, NY), x, c, z)

    def zdev(d):
        return dev(y, x, c, lax.rem(z + d, NZ))

    def wdev(d, across_x):
        return (lax.rem(y + d, NY) * NK + (k_far if across_x else k), plane)

    def remote(src, dst, send, recv, device):
        return pltpu.make_async_remote_copy(
            src_ref=src, dst_ref=dst, send_sem=send, recv_sem=recv, device_id=device, device_id_type=MESH
        )

    own_copy = pltpu.make_async_copy(owner_hbm, owner_ref, in_sem.at[8])
    pool_copy = pltpu.make_async_copy(pool_hbm, pool_ref, in_sem.at[9])
    own_copy.start()
    pool_copy.start()
    CHUNKS = 4
    per = NB // CHUNKS
    loads = []
    for i in range(CHUNKS):
        part = pl.ds(i * per, per)
        lg = pltpu.make_async_copy(g_hbm.at[part], gbuf.at[part], in_sem.at[2 * i])
        lm = pltpu.make_async_copy(m_hbm.at[part], mbuf.at[part], in_sem.at[2 * i + 1])
        lg.start()
        lm.start()
        loads.append((lg, lm))

    barrier = pltpu.get_barrier_semaphore()

    def greet(device):
        pl.semaphore_signal(barrier, inc=1, device_id=device, device_id_type=MESH)

    for d in range(1, NZ):
        greet(zdev(d))
    for d in range(1, NY):
        greet(ydev(d))
    for d in range(1, NX):
        greet(xdev(d))
    greet(partner)

    own_copy.wait()
    pool_copy.wait()
    codes = [pool_ref[0, j] for j in range(NB)]

    def source(q):
        at = jnp.int32(0)
        for j in range(1, NB):
            at = jnp.where(codes[j] == q, j, at)
        return at

    for pair in loads:
        for cp in pair:
            cp.wait()

    def nesterov(j):
        grad = gbuf[j].astype(jnp.float32)
        velocity = momentum_rate * mbuf[j].astype(jnp.float32) + grad
        return velocity, (grad + momentum_rate * velocity).astype(jnp.bfloat16)

    def make_pair(core, at):
        p = lax.rem(2 * at + core + NZ - z, NZ)
        grams = []
        for e in range(2):
            q = 2 * p + e
            _, value = nesterov(source(q))
            yq[q] = value
            wide = value.astype(jnp.float32)
            t0[pl.ds(q, 1), :] = jnp.sum(wide * wide, axis=0, keepdims=True)
            grams.append(
                lax.dot_general(value, value, (((1,), (1,)), ((), ())), preferred_element_type=jnp.float32)
            )
        put_packed(pk.at[core, at], *grams)

    sent = []

    def go(copy):
        copy.start()
        sent.append(copy)
        return copy

    left, right, far = lax.rem(x + NX - 1, NX), lax.rem(x + 1, NX), lax.rem(x + 2, NX)
    order = [far, left, right, x]
    cc = []
    for i, at in enumerate(order):
        make_pair(1 - c, at)
        if i == 0:
            pl.semaphore_wait(barrier, (NZ - 1) + (NY - 1) + (NX - 1) + 1)
        cc.append(go(remote(pk.at[1 - c, at], r0.at[at], c_send.at[i], c_recv.at[i], partner)))
    for at in order:
        make_pair(c, at)
    ct = go(remote(t0, t0r, c_send.at[NX], c_recv.at[NX], partner))

    zc = []
    for d in sorted(range(1, NZ), key=lambda d: -min(d, NZ - d)):
        to = lax.rem(z + d, NZ)
        zc.append(go(remote(yq.at[pl.ds(2 * to, 2)], yr.at[pl.ds(2 * z, 2)], z_send.at[d], z_recv.at[d], zdev(d))))
    mine = pltpu.make_async_copy(yq.at[pl.ds(2 * z, 2)], yr.at[pl.ds(2 * z, 2)], z_recv.at[0])
    mine.start()

    upper, lower = pl.ds(0, H // 2), pl.ds(H // 2, PACKED - H // 2)
    to_right = {"device": dev(y, right, c, z)}
    to_left = {"device": dev(y, left, c, z)}
    cc[0].wait_recv()
    s1[far] = pk[c, far] + r0[far]
    f_up = go(remote(s1.at[far, upper], r1.at[0, upper], x_send.at[0], x_recv.at[0], **to_right))
    f_low = go(remote(s1.at[far, lower], r1.at[0, lower], x_send.at[1], x_recv.at[1], **to_left))
    cc[1].wait_recv()
    s1[left] = pk[c, left] + r0[left]
    d_up = go(remote(s1.at[left, upper], r1.at[1, upper], x_send.at[2], x_recv.at[2], **to_left))
    cc[2].wait_recv()
    s1[right] = pk[c, right] + r0[right]
    d_low = go(remote(s1.at[right, lower], r1.at[1, lower], x_send.at[3], x_recv.at[3], **to_right))
    ct.wait_recv()
    t1[...] = t0[...] + t0r[...]
    tx = [go(remote(t1, t1r.at[d - 1], t_send.at[d], t_recv.at[d], xdev(d))) for d in range(1, NX)]
    cc[3].wait_recv()
    s1[x] = pk[c, x] + r0[x]
    f_up.wait_recv()
    r0[0, upper, :] = s1[right, upper, :] + r1[0, upper, :]
    g_up = go(remote(r0.at[0, upper], r1.at[2, upper], x_send.at[4], x_recv.at[4], **to_right))
    f_low.wait_recv()
    r0[0, lower, :] = s1[left, lower, :] + r1[0, lower, :]
    g_low = go(remote(r0.at[0, lower], r1.at[2, lower], x_send.at[5], x_recv.at[5], **to_left))

    for j in range(NB):
        nm_ref[j] = nesterov(j)[0].astype(jnp.bfloat16)

    for cp in (d_up, d_low, g_up, g_low):
        cp.wait_recv()
    s2[...] = s1[x] + r1[1] + r1[2]
    yc, yd = [], []
    for d in sorted(range(1, NY), key=lambda d: -min(d, NY - d)):
        to = lax.rem(y + d, NY)
        rows = pl.ds(pl.multiple_of(to * CH, CH), CH)
        yc.append(go(remote(s2.at[rows], r2.at[d - 1], y_send.at[d], y_recv.at[d], ydev(d))))
    for d in range(1, NY):
        yd.append(go(remote(s2.at[pl.ds(H, 8)], rd.at[d - 1], y_send.at[NY + d], y_recv.at[NY + d], ydev(d))))
    for cp in tx:
        cp.wait_recv()
    ttotal = t1[...]
    for d in range(1, NX):
        ttotal = ttotal + t1r[d - 1]
    t2[...] = ttotal
    ty = [go(remote(t2, t2r.at[d - 1], t_send.at[NX + d], t_recv.at[NX + d], ydev(d))) for d in range(1, NY)]

    for cp in yc:
        cp.wait_recv()
    total = s2[pl.ds(pl.multiple_of(y * CH, CH), CH), :]
    for d in range(1, NY):
        total = total + r2[d - 1]
    s3[...] = total
    own_rows = pl.ds(pl.multiple_of(y * CH, CH), CH)
    wc = []
    for d in sorted(range(1, NY), key=lambda d: -min(d, NY - d)):
        for i in (1, 0):
            wc.append(
                go(remote(s3, gram.at[i, own_rows], w_send.at[i, d], w_recv.at[i, d], wdev(d, i)))
            )
    wc.append(go(remote(s3, gram.at[1, own_rows], w_send.at[1, 0], w_recv.at[1, 0], wdev(0, 1))))
    for cp in yd:
        cp.wait_recv()
    total = s2[pl.ds(H, 8), :]
    for d in range(1, NY):
        total = total + rd[d - 1]
    sd[...] = total
    last = pl.ds(H, 8)
    wc.append(go(remote(sd, gram.at[1, last], w_send.at[1, NY], w_recv.at[1, NY], wdev(0, 1))))
    w0 = remote(s3, gram.at[0, own_rows], w_send.at[0, 0], w_recv.at[0, 0], wdev(0, 0))
    w1 = remote(sd, gram.at[0, last], w_send.at[0, NY], w_recv.at[0, NY], wdev(0, 0))
    l0 = pltpu.make_async_copy(s3, gram.at[0, own_rows], w_recv.at[0, 0])
    l1 = pltpu.make_async_copy(sd, gram.at[0, last], w_recv.at[0, NY])

    @pl.when(plane != z)
    def _():
        w0.start()
        w1.start()

    @pl.when(plane == z)
    def _():
        l0.start()
        l1.start()

    for cp in ty:
        cp.wait_recv()
    ttotal = t2[...]
    for d in range(1, NY):
        ttotal = ttotal + t2r[d - 1]
    t2r[NY - 1] = ttotal
    count = jnp.int32(0)
    picked = [jnp.zeros((1, H), jnp.float32), jnp.zeros((1, H), jnp.float32)]
    for j in range(NB):
        same = jnp.where(owner_ref[0, j] == f, 1, 0)
        line = t2r[NY - 1, pl.ds(codes[j], 1), :]
        for s in range(2):
            weight = jnp.where(count == s, same, 0).astype(jnp.float32)
            picked[s] = picked[s] + line * weight
        count = count + same
    lane = lax.broadcasted_iota(jnp.int32, (1, 2), 1)
    sums = [jnp.sum(v, axis=1, keepdims=True) for v in picked]
    elements = H * H * NK * NY
    slot_ref[...] = jnp.sqrt(jnp.where(lane == 0, sums[0], sums[1]) / elements)

    for cp in wc:
        cp.wait_recv()
    l0.wait()
    l1.wait()
    qs = newton_schulz([*get_packed(gram.at[0]), *get_packed(gram.at[1])])
    put_packed(qall.at[k], qs[0], qs[1])

    def across(at, i):
        return go(remote(qall.at[at], qall.at[at], b_send.at[i], b_recv.at[i], partner))

    k_left, k_right = 2 * left + c, 2 * right + c
    from_left = go(remote(qall.at[k], qall.at[k], a_send.at[0], a_recv.at[0], to_right["device"]))
    from_right = go(remote(qall.at[k], qall.at[k], a_send.at[1], a_recv.at[1], to_left["device"]))
    b_own = across(k, 0)
    put_packed(qall.at[k_far], qs[2], qs[3])
    b_far = across(k_far, 1)

    mine.wait()
    for cp in zc:
        cp.wait_recv()
    factor = step_size * 0.2 * math.sqrt(H * NK * NY)

    def apply(at):
        slot = lax.rem(at + NZ - z, NZ)
        for e, q in enumerate(get_packed(qall.at[at])):
            high = q.astype(jnp.bfloat16)
            rest = (q - high.astype(jnp.float32)).astype(jnp.bfloat16)
            value = yr[2 * slot + e]
            ortho = jnp.dot(
                jnp.concatenate([high, rest], axis=1),
                jnp.concatenate([value, value], axis=0),
                preferred_element_type=jnp.float32,
            ).astype(jnp.bfloat16)
            out_ref[2 * slot + e] = (-factor * ortho.astype(jnp.float32)).astype(jnp.bfloat16)

    apply(k)
    apply(k_far)
    b_own.wait_recv()
    apply(2 * x + 1 - c)
    b_far.wait_recv()
    apply(2 * far + 1 - c)
    from_left.wait_recv()
    b_left = across(k_left, 2)
    from_right.wait_recv()
    b_right = across(k_right, 3)
    apply(k_left)
    apply(k_right)
    b_left.wait_recv()
    apply(2 * left + 1 - c)
    b_right.wait_recv()
    apply(2 * right + 1 - c)

    for cp in sent:
        cp.wait_send()

    @pl.when(plane != z)
    def _():
        w0.wait_send()
        w1.wait_send()


def writer(*refs):
    copies = [pltpu.make_async_copy(refs[i], refs[3 + i], refs[6].at[i]) for i in range(3)]
    for cp in copies:
        cp.start()
    for cp in copies:
        cp.wait()


def written(results):
    vmem = pl.BlockSpec(memory_space=pltpu.VMEM)
    return pl.pallas_call(
        writer,
        out_shape=tuple(jax.ShapeDtypeStruct(v.shape, v.dtype) for v in results),
        in_specs=[vmem] * 3,
        out_specs=(pl.BlockSpec(memory_space=pltpu.HBM),) * 3,
        scratch_shapes=[pltpu.SemaphoreType.DMA((3,))],
        compiler_params=pltpu.CompilerParams(vmem_limit_bytes=8 * 1024 * 1024),
    )(*results)


def local(sizes, grads, momentum, owner_table, pool_map):
    NX, NY, NZ, NB = sizes
    NK = 2 * NX
    f32, bf16 = jnp.float32, jnp.bfloat16
    dma = pltpu.SemaphoreType.DMA
    hbm = pl.BlockSpec(memory_space=pltpu.HBM)
    scratch = [
        pltpu.SMEM((1, NB), jnp.int32),
        pltpu.SMEM((1, NB), jnp.int32),
        pltpu.VMEM((NB, H, H), bf16),
        pltpu.VMEM((NB, H, H), bf16),
        pltpu.VMEM((NB, H, H), bf16),
        pltpu.VMEM((NB, H, H), bf16),
        pltpu.VMEM((2, NX, PACKED, H), f32),
        pltpu.VMEM((NX, PACKED, H), f32),
        pltpu.VMEM((NX, PACKED, H), f32),
        pltpu.VMEM((NX - 1, PACKED, H), f32),
        pltpu.VMEM((PACKED, H), f32),
        pltpu.VMEM((NY - 1, H // NY, H), f32),
        pltpu.VMEM((NY - 1, 8, H), f32),
        pltpu.VMEM((H // NY, H), f32),
        pltpu.VMEM((8, H), f32),
        pltpu.VMEM((2, PACKED, H), f32),
        pltpu.VMEM((NK, PACKED, H), f32),
        pltpu.VMEM((NB, H), f32),
        pltpu.VMEM((NB, H), f32),
        pltpu.VMEM((NB, H), f32),
        pltpu.VMEM((NX - 1, NB, H), f32),
        pltpu.VMEM((NB, H), f32),
        pltpu.VMEM((NY, NB, H), f32),
        dma((10,)),
        dma((NZ,)),
        dma((NZ,)),
        dma((NX + 1,)),
        dma((NX + 1,)),
        dma((6,)),
        dma((6,)),
        dma((2 * NY,)),
        dma((2 * NY,)),
        dma((NX + NY,)),
        dma((NX + NY,)),
        dma((2, NY + 1)),
        dma((2, NY + 1)),
        dma((2,)),
        dma((2,)),
        dma((NX,)),
        dma((NX,)),
    ]
    results = pl.pallas_call(
        functools.partial(kernel, sizes),
        out_shape=(
            jax.ShapeDtypeStruct(grads.shape, bf16),
            jax.ShapeDtypeStruct(grads.shape, bf16),
            jax.ShapeDtypeStruct((1, 2), f32),
        ),
        in_specs=[hbm] * 4,
        out_specs=(pl.BlockSpec(memory_space=pltpu.VMEM),) * 3,
        scratch_shapes=scratch,
        compiler_params=pltpu.CompilerParams(
            collective_id=0, has_side_effects=True, vmem_limit_bytes=24 * 1024 * 1024
        ),
    )(
        *(
            pltpu.with_memory_space_constraint(v, pltpu.HBM)
            for v in (owner_table.reshape(1, NB), pool_map, grads, momentum)
        )
    )
    return written(results)


def solution(mesh, sizes=(4, 8, 8, 16)):
    in_specs = (P("tp", None, "fsdp"), P("tp", None, "fsdp"), P("tp", None), P("tp", None))
    out_specs = (P("tp", None, "fsdp"), P("tp", None, "fsdp"), P("tp", "fsdp"))
    return jax.shard_map(
        functools.partial(local, sizes), mesh=mesh, in_specs=in_specs, out_specs=out_specs, check_vma=False
    )
```

```python
import functools
import math

import jax
import jax.numpy as jnp
from jax import lax
from jax.experimental import pallas as pl
from jax.experimental.pallas import tpu as pltpu
from jax.sharding import PartitionSpec as P

ITERS = 3
momentum_rate = 0.95
step_size = 0.8
epsilon = 1e-07
poly_linear = 3.4445
poly_cubic = -4.775
poly_quintic = 2.0315

H = 128
PACKED = H + 8
MESH = pl.DeviceIdType.MESH


def masks():
    row = lax.broadcasted_iota(jnp.int32, (H, H), 0)
    col = lax.broadcasted_iota(jnp.int32, (H, H), 1)
    return row >= col, row == col


def put_packed(ref, a, b):
    low, diag = masks()
    ref[0:H, :] = jnp.where(low, a, b)
    last = jnp.sum(jnp.where(diag, b, 0.0), axis=0, keepdims=True)
    ref[H:PACKED, :] = jnp.broadcast_to(last, (8, H))


def get_packed(ref):
    low, diag = masks()
    both = ref[0:H, :]
    other = both.T
    last = jnp.broadcast_to(ref[H : H + 1, :], (H, H))
    a = jnp.where(low, both, other)
    b = jnp.where(diag, last, jnp.where(low, other, both))
    return a, b


def halves(v):
    high = v.astype(jnp.bfloat16)
    return high, (v - high.astype(jnp.float32)).astype(jnp.bfloat16)


def dot32(a, b):
    (ah, al), (bh, bl) = halves(a), halves(b)
    return jnp.dot(
        jnp.concatenate([ah, al, ah], axis=1),
        jnp.concatenate([bh, bh, bl], axis=0),
        preferred_element_type=jnp.float32,
    )


def newton_schulz(grams):
    _, diag = masks()
    identity = jnp.where(diag, 1.0, 0.0)
    inverses, gs, qs = [], [], [None] * len(grams)
    for g in grams:
        squares = jnp.sum(jnp.where(diag, g, 0.0), keepdims=True)
        inverse = 1.0 / (jnp.sqrt(squares) + epsilon)
        inverses.append(inverse)
        gs.append(g * (inverse * inverse))
    for it in range(ITERS):
        g2 = [dot32(g, g) for g in gs]
        ms = [poly_linear * identity + poly_cubic * g + poly_quintic * s for g, s in zip(gs, g2)]
        if it < ITERS - 1:
            right = [dot32(g, m) for g, m in zip(gs, ms)]
        qs = [m if it == 0 else dot32(m, q) for m, q in zip(ms, qs)]
        if it < ITERS - 1:
            gs = [dot32(m, r) for m, r in zip(ms, right)]
    return [q * inverse for q, inverse in zip(qs, inverses)]


def kernel(
    sizes,
    owner_hbm,
    pool_hbm,
    g_hbm,
    m_hbm,
    nm_ref,
    out_ref,
    slot_ref,
    owner_ref,
    pool_ref,
    gbuf,
    mbuf,
    yq,
    yr,
    pk,
    r0,
    s1,
    r1,
    s2,
    r2,
    rd,
    s3,
    sd,
    gram,
    qall,
    t0,
    t0r,
    t1,
    t1r,
    t2,
    t2r,
    in_sem,
    z_send,
    z_recv,
    c_send,
    c_recv,
    x_send,
    x_recv,
    y_send,
    y_recv,
    t_send,
    t_recv,
    w_send,
    w_recv,
    a_send,
    a_recv,
    b_send,
    b_recv,
):
    NX, NY, NZ, NB = sizes
    NK = 2 * NX
    CH = H // NY
    f = lax.axis_index("fsdp")
    z = lax.axis_index("tp")
    k = lax.rem(f, NK)
    y = lax.div(f, NK)
    x = lax.div(k, 2)
    c = lax.rem(k, 2)
    plane = lax.rem(k + NZ - z, NZ)

    def dev(yy, xx, cc, zz):
        return ((yy * NX + xx) * 2 + cc, zz)

    partner = dev(y, x, 1 - c, z)

    def xdev(d):
        return dev(y, lax.rem(x + d, NX), c, z)

    def ydev(d):
        return dev(lax.rem(y + d, NY), x, c, z)

    def zdev(d):
        return dev(y, x, c, lax.rem(z + d, NZ))

    def wdev(d):
        return (lax.rem(y + d, NY) * NK + k, plane)

    def remote(src, dst, send, recv, device):
        return pltpu.make_async_remote_copy(
            src_ref=src, dst_ref=dst, send_sem=send, recv_sem=recv, device_id=device, device_id_type=MESH
        )

    own_copy = pltpu.make_async_copy(owner_hbm, owner_ref, in_sem.at[8])
    pool_copy = pltpu.make_async_copy(pool_hbm, pool_ref, in_sem.at[9])
    own_copy.start()
    pool_copy.start()
    CHUNKS = 4
    per = NB // CHUNKS
    loads = []
    for i in range(CHUNKS):
        part = pl.ds(i * per, per)
        lg = pltpu.make_async_copy(g_hbm.at[part], gbuf.at[part], in_sem.at[2 * i])
        lm = pltpu.make_async_copy(m_hbm.at[part], mbuf.at[part], in_sem.at[2 * i + 1])
        lg.start()
        lm.start()
        loads.append((lg, lm))

    barrier = pltpu.get_barrier_semaphore()

    def greet(device):
        pl.semaphore_signal(barrier, inc=1, device_id=device, device_id_type=MESH)

    for d in range(1, NZ):
        greet(zdev(d))
    for d in range(1, NY):
        greet(ydev(d))
    for d in range(1, NX):
        greet(xdev(d))
    greet(partner)

    own_copy.wait()
    pool_copy.wait()
    codes = [pool_ref[0, j] for j in range(NB)]

    def source(q):
        at = jnp.int32(0)
        for j in range(1, NB):
            at = jnp.where(codes[j] == q, j, at)
        return at

    for pair in loads:
        for cp in pair:
            cp.wait()

    def nesterov(j):
        grad = gbuf[j].astype(jnp.float32)
        velocity = momentum_rate * mbuf[j].astype(jnp.float32) + grad
        return velocity, (grad + momentum_rate * velocity).astype(jnp.bfloat16)

    def make_pair(core, at):
        p = lax.rem(2 * at + core + NZ - z, NZ)
        grams = []
        for e in range(2):
            q = 2 * p + e
            _, value = nesterov(source(q))
            yq[q] = value
            wide = value.astype(jnp.float32)
            t0[pl.ds(q, 1), :] = jnp.sum(wide * wide, axis=0, keepdims=True)
            grams.append(
                lax.dot_general(value, value, (((1,), (1,)), ((), ())), preferred_element_type=jnp.float32)
            )
        put_packed(pk.at[core, at], *grams)

    sent = []

    def go(copy):
        copy.start()
        sent.append(copy)
        return copy

    left, right, far = lax.rem(x + NX - 1, NX), lax.rem(x + 1, NX), lax.rem(x + 2, NX)
    order = [far, left, right, x]
    cc = []
    for i, at in enumerate(order):
        make_pair(1 - c, at)
        if i == 0:
            pl.semaphore_wait(barrier, (NZ - 1) + (NY - 1) + (NX - 1) + 1)
        cc.append(go(remote(pk.at[1 - c, at], r0.at[at], c_send.at[i], c_recv.at[i], partner)))
    for at in order:
        make_pair(c, at)
    ct = go(remote(t0, t0r, c_send.at[NX], c_recv.at[NX], partner))

    zc = []
    for d in sorted(range(1, NZ), key=lambda d: -min(d, NZ - d)):
        to = lax.rem(z + d, NZ)
        zc.append(go(remote(yq.at[pl.ds(2 * to, 2)], yr.at[pl.ds(2 * z, 2)], z_send.at[d], z_recv.at[d], zdev(d))))
    mine = pltpu.make_async_copy(yq.at[pl.ds(2 * z, 2)], yr.at[pl.ds(2 * z, 2)], z_recv.at[0])
    mine.start()

    upper, lower = pl.ds(0, H // 2), pl.ds(H // 2, PACKED - H // 2)
    to_right = {"device": dev(y, right, c, z)}
    to_left = {"device": dev(y, left, c, z)}
    xc = []
    for i, d in enumerate((2, 3, 1)):
        cc[i].wait_recv()
        at = order[i]
        s1[at] = pk[c, at] + r0[at]
        xc.append(go(remote(s1.at[at], r1.at[d - 1], x_send.at[d], x_recv.at[d], xdev(d))))
    ct.wait_recv()
    t1[...] = t0[...] + t0r[...]
    tx = [go(remote(t1, t1r.at[d - 1], t_send.at[d], t_recv.at[d], xdev(d))) for d in range(1, NX)]
    cc[3].wait_recv()
    s1[x] = pk[c, x] + r0[x]

    for j in range(NB):
        nm_ref[j] = nesterov(j)[0].astype(jnp.bfloat16)

    for cp in xc:
        cp.wait_recv()
    s2[...] = s1[x] + r1[0] + r1[1] + r1[2]
    yc, yd = [], []
    for d in sorted(range(1, NY), key=lambda d: -min(d, NY - d)):
        to = lax.rem(y + d, NY)
        rows = pl.ds(pl.multiple_of(to * CH, CH), CH)
        yc.append(go(remote(s2.at[rows], r2.at[d - 1], y_send.at[d], y_recv.at[d], ydev(d))))
    for d in range(1, NY):
        yd.append(go(remote(s2.at[pl.ds(H, 8)], rd.at[d - 1], y_send.at[NY + d], y_recv.at[NY + d], ydev(d))))
    for cp in tx:
        cp.wait_recv()
    ttotal = t1[...]
    for d in range(1, NX):
        ttotal = ttotal + t1r[d - 1]
    t2[...] = ttotal
    ty = [go(remote(t2, t2r.at[d - 1], t_send.at[NX + d], t_recv.at[NX + d], ydev(d))) for d in range(1, NY)]

    for cp in yc:
        cp.wait_recv()
    total = s2[pl.ds(pl.multiple_of(y * CH, CH), CH), :]
    for d in range(1, NY):
        total = total + r2[d - 1]
    s3[...] = total
    own_rows = pl.ds(pl.multiple_of(y * CH, CH), CH)
    wc = []
    for d in sorted(range(1, NY), key=lambda d: -min(d, NY - d)):
        wc.append(go(remote(s3, gram.at[own_rows], w_send.at[d], w_recv.at[d], wdev(d))))
    for cp in yd:
        cp.wait_recv()
    total = s2[pl.ds(H, 8), :]
    for d in range(1, NY):
        total = total + rd[d - 1]
    sd[...] = total
    w0 = remote(s3, gram.at[own_rows], w_send.at[0], w_recv.at[0], wdev(0))
    w1 = remote(sd, gram.at[pl.ds(H, 8)], w_send.at[NY], w_recv.at[NY], wdev(0))
    l0 = pltpu.make_async_copy(s3, gram.at[own_rows], w_recv.at[0])
    l1 = pltpu.make_async_copy(sd, gram.at[pl.ds(H, 8)], w_recv.at[NY])

    @pl.when(plane != z)
    def _():
        w0.start()
        w1.start()

    @pl.when(plane == z)
    def _():
        l0.start()
        l1.start()

    for cp in ty:
        cp.wait_recv()
    ttotal = t2[...]
    for d in range(1, NY):
        ttotal = ttotal + t2r[d - 1]
    t2r[NY - 1] = ttotal
    count = jnp.int32(0)
    picked = [jnp.zeros((1, H), jnp.float32), jnp.zeros((1, H), jnp.float32)]
    for j in range(NB):
        same = jnp.where(owner_ref[0, j] == f, 1, 0)
        line = t2r[NY - 1, pl.ds(codes[j], 1), :]
        for s in range(2):
            weight = jnp.where(count == s, same, 0).astype(jnp.float32)
            picked[s] = picked[s] + line * weight
        count = count + same
    lane = lax.broadcasted_iota(jnp.int32, (1, 2), 1)
    sums = [jnp.sum(v, axis=1, keepdims=True) for v in picked]
    elements = H * H * NK * NY
    slot_ref[...] = jnp.sqrt(jnp.where(lane == 0, sums[0], sums[1]) / elements)

    for cp in wc:
        cp.wait_recv()
    l0.wait()
    l1.wait()
    a, b = newton_schulz(list(get_packed(gram)))
    put_packed(qall.at[k], a, b)

    b_own = go(remote(qall.at[k], qall.at[k], b_send.at[0], b_recv.at[0], partner))
    xa = {}
    for d in (2, 1, 3):
        xa[d] = go(remote(qall.at[k], qall.at[k], a_send.at[d], a_recv.at[d], xdev(d)))

    mine.wait()
    for cp in zc:
        cp.wait_recv()
    factor = step_size * 0.2 * math.sqrt(H * NK * NY)

    def apply(at):
        slot = lax.rem(at + NZ - z, NZ)
        for e, q in enumerate(get_packed(qall.at[at])):
            high = q.astype(jnp.bfloat16)
            rest = (q - high.astype(jnp.float32)).astype(jnp.bfloat16)
            value = yr[2 * slot + e]
            ortho = jnp.dot(
                jnp.concatenate([high, rest], axis=1),
                jnp.concatenate([value, value], axis=0),
                preferred_element_type=jnp.float32,
            ).astype(jnp.bfloat16)
            out_ref[2 * slot + e] = (-factor * ortho.astype(jnp.float32)).astype(jnp.bfloat16)

    def across(at, i):
        return go(remote(qall.at[at], qall.at[at], b_send.at[i], b_recv.at[i], partner))

    apply(k)
    b_own.wait_recv()
    apply(2 * x + 1 - c)
    fwd = {}
    for d in (1, 3, 2):
        xa[d].wait_recv()
        at = 2 * lax.rem(x + NX - d, NX) + c
        fwd[d] = go(remote(qall.at[at], qall.at[at], b_send.at[d], b_recv.at[d], partner))
        apply(at)
    for d in (1, 3, 2):
        fwd[d].wait_recv()
        apply(2 * lax.rem(x + NX - d, NX) + 1 - c)

    for cp in sent:
        cp.wait_send()

    @pl.when(plane != z)
    def _():
        w0.wait_send()
        w1.wait_send()


def writer(*refs):
    copies = [pltpu.make_async_copy(refs[i], refs[3 + i], refs[6].at[i]) for i in range(3)]
    for cp in copies:
        cp.start()
    for cp in copies:
        cp.wait()


def written(results):
    vmem = pl.BlockSpec(memory_space=pltpu.VMEM)
    return pl.pallas_call(
        writer,
        out_shape=tuple(jax.ShapeDtypeStruct(v.shape, v.dtype) for v in results),
        in_specs=[vmem] * 3,
        out_specs=(pl.BlockSpec(memory_space=pltpu.HBM),) * 3,
        scratch_shapes=[pltpu.SemaphoreType.DMA((3,))],
        compiler_params=pltpu.CompilerParams(vmem_limit_bytes=8 * 1024 * 1024),
    )(*results)


def local(sizes, grads, momentum, owner_table, pool_map):
    NX, NY, NZ, NB = sizes
    NK = 2 * NX
    f32, bf16 = jnp.float32, jnp.bfloat16
    dma = pltpu.SemaphoreType.DMA
    hbm = pl.BlockSpec(memory_space=pltpu.HBM)
    scratch = [
        pltpu.SMEM((1, NB), jnp.int32),
        pltpu.SMEM((1, NB), jnp.int32),
        pltpu.VMEM((NB, H, H), bf16),
        pltpu.VMEM((NB, H, H), bf16),
        pltpu.VMEM((NB, H, H), bf16),
        pltpu.VMEM((NB, H, H), bf16),
        pltpu.VMEM((2, NX, PACKED, H), f32),
        pltpu.VMEM((NX, PACKED, H), f32),
        pltpu.VMEM((NX, PACKED, H), f32),
        pltpu.VMEM((NX - 1, PACKED, H), f32),
        pltpu.VMEM((PACKED, H), f32),
        pltpu.VMEM((NY - 1, H // NY, H), f32),
        pltpu.VMEM((NY - 1, 8, H), f32),
        pltpu.VMEM((H // NY, H), f32),
        pltpu.VMEM((8, H), f32),
        pltpu.VMEM((PACKED, H), f32),
        pltpu.VMEM((NK, PACKED, H), f32),
        pltpu.VMEM((NB, H), f32),
        pltpu.VMEM((NB, H), f32),
        pltpu.VMEM((NB, H), f32),
        pltpu.VMEM((NX - 1, NB, H), f32),
        pltpu.VMEM((NB, H), f32),
        pltpu.VMEM((NY, NB, H), f32),
        dma((10,)),
        dma((NZ,)),
        dma((NZ,)),
        dma((NX + 1,)),
        dma((NX + 1,)),
        dma((6,)),
        dma((6,)),
        dma((2 * NY,)),
        dma((2 * NY,)),
        dma((NX + NY,)),
        dma((NX + NY,)),
        dma((NY + 1,)),
        dma((NY + 1,)),
        dma((6,)),
        dma((6,)),
        dma((NX,)),
        dma((NX,)),
    ]
    results = pl.pallas_call(
        functools.partial(kernel, sizes),
        out_shape=(
            jax.ShapeDtypeStruct(grads.shape, bf16),
            jax.ShapeDtypeStruct(grads.shape, bf16),
            jax.ShapeDtypeStruct((1, 2), f32),
        ),
        in_specs=[hbm] * 4,
        out_specs=(pl.BlockSpec(memory_space=pltpu.VMEM),) * 3,
        scratch_shapes=scratch,
        compiler_params=pltpu.CompilerParams(
            collective_id=0, has_side_effects=True, vmem_limit_bytes=24 * 1024 * 1024
        ),
    )(
        *(
            pltpu.with_memory_space_constraint(v, pltpu.HBM)
            for v in (owner_table.reshape(1, NB), pool_map, grads, momentum)
        )
    )
    return written(results)


def solution(mesh, sizes=(4, 8, 8, 16)):
    in_specs = (P("tp", None, "fsdp"), P("tp", None, "fsdp"), P("tp", None), P("tp", None))
    out_specs = (P("tp", None, "fsdp"), P("tp", None, "fsdp"), P("tp", "fsdp"))
    return jax.shard_map(
        functools.partial(local, sizes), mesh=mesh, in_specs=in_specs, out_specs=out_specs, check_vma=False
    )
```

```python
import functools
import math

import jax
import jax.numpy as jnp
from jax import lax
from jax.experimental import pallas as pl
from jax.experimental.pallas import tpu as pltpu
from jax.sharding import PartitionSpec as P

ITERS = 3
momentum_rate = 0.95
step_size = 0.8
epsilon = 1e-07
poly_linear = 3.4445
poly_cubic = -4.775
poly_quintic = 2.0315

H = 128
PACKED = H + 8
MESH = pl.DeviceIdType.MESH


def masks():
    row = lax.broadcasted_iota(jnp.int32, (H, H), 0)
    col = lax.broadcasted_iota(jnp.int32, (H, H), 1)
    return row >= col, row == col


def put_packed(ref, a, b):
    low, diag = masks()
    ref[0:H, :] = jnp.where(low, a, b)
    last = jnp.sum(jnp.where(diag, b, 0.0), axis=0, keepdims=True)
    ref[H:PACKED, :] = jnp.broadcast_to(last, (8, H))


def get_packed(ref):
    low, diag = masks()
    both = ref[0:H, :]
    other = both.T
    last = jnp.broadcast_to(ref[H : H + 1, :], (H, H))
    a = jnp.where(low, both, other)
    b = jnp.where(diag, last, jnp.where(low, other, both))
    return a, b


def halves(v):
    high = v.astype(jnp.bfloat16)
    return high, (v - high.astype(jnp.float32)).astype(jnp.bfloat16)


def dot32(a, b):
    (ah, al), (bh, bl) = halves(a), halves(b)
    return jnp.dot(
        jnp.concatenate([ah, al, ah], axis=1),
        jnp.concatenate([bh, bh, bl], axis=0),
        preferred_element_type=jnp.float32,
    )


def newton_schulz(grams):
    _, diag = masks()
    identity = jnp.where(diag, 1.0, 0.0)
    inverses, gs, qs = [], [], [None] * len(grams)
    for g in grams:
        squares = jnp.sum(jnp.where(diag, g, 0.0), keepdims=True)
        inverse = 1.0 / (jnp.sqrt(squares) + epsilon)
        inverses.append(inverse)
        gs.append(g * (inverse * inverse))
    for it in range(ITERS):
        g2 = [dot32(g, g) for g in gs]
        ms = [poly_linear * identity + poly_cubic * g + poly_quintic * s for g, s in zip(gs, g2)]
        if it < ITERS - 1:
            right = [dot32(g, m) for g, m in zip(gs, ms)]
        qs = [m if it == 0 else dot32(m, q) for m, q in zip(ms, qs)]
        if it < ITERS - 1:
            gs = [dot32(m, r) for m, r in zip(ms, right)]
    return [q * inverse for q, inverse in zip(qs, inverses)]


def kernel(
    sizes,
    owner_hbm,
    pool_hbm,
    g_hbm,
    m_hbm,
    nm_ref,
    out_ref,
    slot_ref,
    owner_ref,
    pool_ref,
    gbuf,
    mbuf,
    yq,
    yr,
    pk,
    r0,
    s1,
    r1,
    s2,
    r2,
    rd,
    s3,
    sd,
    gram,
    qall,
    t0,
    t0r,
    t1,
    t1r,
    t2,
    t2r,
    in_sem,
    z_send,
    z_recv,
    c_send,
    c_recv,
    x_send,
    x_recv,
    y_send,
    y_recv,
    t_send,
    t_recv,
    w_send,
    w_recv,
    a_send,
    a_recv,
    b_send,
    b_recv,
):
    NX, NY, NZ, NB = sizes
    NK = 2 * NX
    CH = H // NY
    f = lax.axis_index("fsdp")
    z = lax.axis_index("tp")
    k = lax.rem(f, NK)
    y = lax.div(f, NK)
    x = lax.div(k, 2)
    c = lax.rem(k, 2)
    plane = lax.rem(k + NZ - z, NZ)

    def dev(yy, xx, cc, zz):
        return ((yy * NX + xx) * 2 + cc, zz)

    partner = dev(y, x, 1 - c, z)

    def xdev(d):
        return dev(y, lax.rem(x + d, NX), c, z)

    def ydev(d):
        return dev(lax.rem(y + d, NY), x, c, z)

    def zdev(d):
        return dev(y, x, c, lax.rem(z + d, NZ))

    def wdev(d):
        return (lax.rem(y + d, NY) * NK + k, plane)

    def remote(src, dst, send, recv, device):
        return pltpu.make_async_remote_copy(
            src_ref=src, dst_ref=dst, send_sem=send, recv_sem=recv, device_id=device, device_id_type=MESH
        )

    own_copy = pltpu.make_async_copy(owner_hbm, owner_ref, in_sem.at[8])
    pool_copy = pltpu.make_async_copy(pool_hbm, pool_ref, in_sem.at[9])
    own_copy.start()
    pool_copy.start()
    CHUNKS = 4
    per = NB // CHUNKS
    loads = []
    for i in range(CHUNKS):
        part = pl.ds(i * per, per)
        lg = pltpu.make_async_copy(g_hbm.at[part], gbuf.at[part], in_sem.at[2 * i])
        lm = pltpu.make_async_copy(m_hbm.at[part], mbuf.at[part], in_sem.at[2 * i + 1])
        lg.start()
        lm.start()
        loads.append((lg, lm))

    barrier = pltpu.get_barrier_semaphore()

    def greet(device):
        pl.semaphore_signal(barrier, inc=1, device_id=device, device_id_type=MESH)

    for d in range(1, NZ):
        greet(zdev(d))
    for d in range(1, NY):
        greet(ydev(d))
    for d in range(1, NX):
        greet(xdev(d))
    greet(partner)

    own_copy.wait()
    pool_copy.wait()
    codes = [pool_ref[0, j] for j in range(NB)]

    def source(q):
        at = jnp.int32(0)
        for j in range(1, NB):
            at = jnp.where(codes[j] == q, j, at)
        return at

    left, right, far = lax.rem(x + NX - 1, NX), lax.rem(x + 1, NX), lax.rem(x + 2, NX)
    order = [far, left, right, x]
    blocks = {}
    for whose, core in (("theirs", 1 - c), ("ours", c)):
        for i, at in enumerate(order):
            p = lax.rem(2 * at + core + NZ - z, NZ)
            blocks[whose, i] = (p, [source(2 * p), source(2 * p + 1)])

    for pair in loads:
        for cp in pair:
            cp.wait()

    def nesterov(j):
        grad = gbuf[j].astype(jnp.float32)
        velocity = momentum_rate * mbuf[j].astype(jnp.float32) + grad
        return velocity, (grad + momentum_rate * velocity).astype(jnp.bfloat16)

    def over_z(d):
        to = lax.rem(z + d, NZ)
        return remote(
            yq.at[pl.ds(2 * to, 2)], yr.at[pl.ds(2 * z, 2)], z_send.at[d], z_recv.at[d], (f, to)
        )

    mine = pltpu.make_async_copy(yq.at[pl.ds(2 * z, 2)], yr.at[pl.ds(2 * z, 2)], z_recv.at[0])

    def send_y(p):
        d = lax.rem(p + NZ - z, NZ)

        @pl.when(d != 0)
        def _():
            over_z(d).start()

        @pl.when(d == 0)
        def _():
            mine.start()

    def make_pair(whose, i):
        core, at = (c if whose == "ours" else 1 - c), order[i]
        p, taken = blocks[whose, i]
        grams = []
        for e in range(2):
            q = 2 * p + e
            _, value = nesterov(taken[e])
            yq[q] = value
            wide = value.astype(jnp.float32)
            t0[pl.ds(q, 1), :] = jnp.sum(wide * wide, axis=0, keepdims=True)
            grams.append(
                lax.dot_general(value, value, (((1,), (1,)), ((), ())), preferred_element_type=jnp.float32)
            )
        put_packed(pk.at[core, at], *grams)

    sent = []

    def go(copy):
        copy.start()
        sent.append(copy)
        return copy

    cc = []
    for i, at in enumerate(order):
        make_pair("theirs", i)
        if i == 0:
            pl.semaphore_wait(barrier, (NZ - 1) + (NY - 1) + (NX - 1) + 1)
        cc.append(go(remote(pk.at[1 - c, at], r0.at[at], c_send.at[i], c_recv.at[i], partner)))
        send_y(blocks["theirs", i][0])
    for i in range(NX):
        make_pair("ours", i)
        send_y(blocks["ours", i][0])
    ct = go(remote(t0, t0r, c_send.at[NX], c_recv.at[NX], partner))

    upper, lower = pl.ds(0, H // 2), pl.ds(H // 2, PACKED - H // 2)
    to_right = {"device": dev(y, right, c, z)}
    to_left = {"device": dev(y, left, c, z)}
    xc = []
    for i, d in enumerate((2, 3, 1)):
        cc[i].wait_recv()
        at = order[i]
        s1[at] = pk[c, at] + r0[at]
        xc.append(go(remote(s1.at[at], r1.at[d - 1], x_send.at[d], x_recv.at[d], xdev(d))))
    ct.wait_recv()
    t1[...] = t0[...] + t0r[...]
    tx = [go(remote(t1, t1r.at[d - 1], t_send.at[d], t_recv.at[d], xdev(d))) for d in range(1, NX)]
    cc[3].wait_recv()
    s1[x] = pk[c, x] + r0[x]

    for j in range(NB):
        nm_ref[j] = nesterov(j)[0].astype(jnp.bfloat16)

    for cp in xc:
        cp.wait_recv()
    s2[...] = s1[x] + r1[0] + r1[1] + r1[2]
    yc, yd = [], []
    for d in sorted(range(1, NY), key=lambda d: -min(d, NY - d)):
        to = lax.rem(y + d, NY)
        rows = pl.ds(pl.multiple_of(to * CH, CH), CH)
        yc.append(go(remote(s2.at[rows], r2.at[d - 1], y_send.at[d], y_recv.at[d], ydev(d))))
    for d in range(1, NY):
        yd.append(go(remote(s2.at[pl.ds(H, 8)], rd.at[d - 1], y_send.at[NY + d], y_recv.at[NY + d], ydev(d))))
    for cp in tx:
        cp.wait_recv()
    ttotal = t1[...]
    for d in range(1, NX):
        ttotal = ttotal + t1r[d - 1]
    t2[...] = ttotal
    ty = [go(remote(t2, t2r.at[d - 1], t_send.at[NX + d], t_recv.at[NX + d], ydev(d))) for d in range(1, NY)]

    for cp in yc:
        cp.wait_recv()
    total = s2[pl.ds(pl.multiple_of(y * CH, CH), CH), :]
    for d in range(1, NY):
        total = total + r2[d - 1]
    s3[...] = total
    own_rows = pl.ds(pl.multiple_of(y * CH, CH), CH)
    wc = []
    for d in sorted(range(1, NY), key=lambda d: -min(d, NY - d)):
        wc.append(go(remote(s3, gram.at[own_rows], w_send.at[d], w_recv.at[d], wdev(d))))
    for cp in yd:
        cp.wait_recv()
    total = s2[pl.ds(H, 8), :]
    for d in range(1, NY):
        total = total + rd[d - 1]
    sd[...] = total
    w0 = remote(s3, gram.at[own_rows], w_send.at[0], w_recv.at[0], wdev(0))
    w1 = remote(sd, gram.at[pl.ds(H, 8)], w_send.at[NY], w_recv.at[NY], wdev(0))
    l0 = pltpu.make_async_copy(s3, gram.at[own_rows], w_recv.at[0])
    l1 = pltpu.make_async_copy(sd, gram.at[pl.ds(H, 8)], w_recv.at[NY])

    @pl.when(plane != z)
    def _():
        w0.start()
        w1.start()

    @pl.when(plane == z)
    def _():
        l0.start()
        l1.start()

    for cp in ty:
        cp.wait_recv()
    ttotal = t2[...]
    for d in range(1, NY):
        ttotal = ttotal + t2r[d - 1]
    t2r[NY - 1] = ttotal
    count = jnp.int32(0)
    picked = [jnp.zeros((1, H), jnp.float32), jnp.zeros((1, H), jnp.float32)]
    for j in range(NB):
        same = jnp.where(owner_ref[0, j] == f, 1, 0)
        line = t2r[NY - 1, pl.ds(codes[j], 1), :]
        for s in range(2):
            weight = jnp.where(count == s, same, 0).astype(jnp.float32)
            picked[s] = picked[s] + line * weight
        count = count + same
    lane = lax.broadcasted_iota(jnp.int32, (1, 2), 1)
    sums = [jnp.sum(v, axis=1, keepdims=True) for v in picked]
    elements = H * H * NK * NY
    slot_ref[...] = jnp.sqrt(jnp.where(lane == 0, sums[0], sums[1]) / elements)

    for cp in wc:
        cp.wait_recv()
    l0.wait()
    l1.wait()
    a, b = newton_schulz(list(get_packed(gram)))
    put_packed(qall.at[k], a, b)

    b_own = go(remote(qall.at[k], qall.at[k], b_send.at[0], b_recv.at[0], partner))
    xa = {}
    for d in (2, 1, 3):
        xa[d] = go(remote(qall.at[k], qall.at[k], a_send.at[d], a_recv.at[d], xdev(d)))

    mine.wait()
    for d in range(1, NZ):
        over_z(d).wait_recv()
    factor = step_size * 0.2 * math.sqrt(H * NK * NY)

    def apply(at):
        slot = lax.rem(at + NZ - z, NZ)
        for e, q in enumerate(get_packed(qall.at[at])):
            high = q.astype(jnp.bfloat16)
            rest = (q - high.astype(jnp.float32)).astype(jnp.bfloat16)
            value = yr[2 * slot + e]
            ortho = jnp.dot(
                jnp.concatenate([high, rest], axis=1),
                jnp.concatenate([value, value], axis=0),
                preferred_element_type=jnp.float32,
            ).astype(jnp.bfloat16)
            out_ref[2 * slot + e] = (-factor * ortho.astype(jnp.float32)).astype(jnp.bfloat16)

    def across(at, i):
        return go(remote(qall.at[at], qall.at[at], b_send.at[i], b_recv.at[i], partner))

    apply(k)
    b_own.wait_recv()
    apply(2 * x + 1 - c)
    fwd = {}
    for d in (1, 3, 2):
        xa[d].wait_recv()
        at = 2 * lax.rem(x + NX - d, NX) + c
        fwd[d] = go(remote(qall.at[at], qall.at[at], b_send.at[d], b_recv.at[d], partner))
        apply(at)
    for d in (1, 3, 2):
        fwd[d].wait_recv()
        apply(2 * lax.rem(x + NX - d, NX) + 1 - c)

    for cp in sent:
        cp.wait_send()
    for d in range(1, NZ):
        over_z(d).wait_send()

    @pl.when(plane != z)
    def _():
        w0.wait_send()
        w1.wait_send()


def writer(*refs):
    copies = [pltpu.make_async_copy(refs[i], refs[3 + i], refs[6].at[i]) for i in range(3)]
    for cp in copies:
        cp.start()
    for cp in copies:
        cp.wait()


def written(results):
    vmem = pl.BlockSpec(memory_space=pltpu.VMEM)
    return pl.pallas_call(
        writer,
        out_shape=tuple(jax.ShapeDtypeStruct(v.shape, v.dtype) for v in results),
        in_specs=[vmem] * 3,
        out_specs=(pl.BlockSpec(memory_space=pltpu.HBM),) * 3,
        scratch_shapes=[pltpu.SemaphoreType.DMA((3,))],
        compiler_params=pltpu.CompilerParams(vmem_limit_bytes=8 * 1024 * 1024),
    )(*results)


def local(sizes, grads, momentum, owner_table, pool_map):
    NX, NY, NZ, NB = sizes
    NK = 2 * NX
    f32, bf16 = jnp.float32, jnp.bfloat16
    dma = pltpu.SemaphoreType.DMA
    hbm = pl.BlockSpec(memory_space=pltpu.HBM)
    scratch = [
        pltpu.SMEM((1, NB), jnp.int32),
        pltpu.SMEM((1, NB), jnp.int32),
        pltpu.VMEM((NB, H, H), bf16),
        pltpu.VMEM((NB, H, H), bf16),
        pltpu.VMEM((NB, H, H), bf16),
        pltpu.VMEM((NB, H, H), bf16),
        pltpu.VMEM((2, NX, PACKED, H), f32),
        pltpu.VMEM((NX, PACKED, H), f32),
        pltpu.VMEM((NX, PACKED, H), f32),
        pltpu.VMEM((NX - 1, PACKED, H), f32),
        pltpu.VMEM((PACKED, H), f32),
        pltpu.VMEM((NY - 1, H // NY, H), f32),
        pltpu.VMEM((NY - 1, 8, H), f32),
        pltpu.VMEM((H // NY, H), f32),
        pltpu.VMEM((8, H), f32),
        pltpu.VMEM((PACKED, H), f32),
        pltpu.VMEM((NK, PACKED, H), f32),
        pltpu.VMEM((NB, H), f32),
        pltpu.VMEM((NB, H), f32),
        pltpu.VMEM((NB, H), f32),
        pltpu.VMEM((NX - 1, NB, H), f32),
        pltpu.VMEM((NB, H), f32),
        pltpu.VMEM((NY, NB, H), f32),
        dma((10,)),
        dma((NZ,)),
        dma((NZ,)),
        dma((NX + 1,)),
        dma((NX + 1,)),
        dma((6,)),
        dma((6,)),
        dma((2 * NY,)),
        dma((2 * NY,)),
        dma((NX + NY,)),
        dma((NX + NY,)),
        dma((NY + 1,)),
        dma((NY + 1,)),
        dma((6,)),
        dma((6,)),
        dma((NX,)),
        dma((NX,)),
    ]
    results = pl.pallas_call(
        functools.partial(kernel, sizes),
        out_shape=(
            jax.ShapeDtypeStruct(grads.shape, bf16),
            jax.ShapeDtypeStruct(grads.shape, bf16),
            jax.ShapeDtypeStruct((1, 2), f32),
        ),
        in_specs=[hbm] * 4,
        out_specs=(pl.BlockSpec(memory_space=pltpu.VMEM),) * 3,
        scratch_shapes=scratch,
        compiler_params=pltpu.CompilerParams(
            collective_id=0, has_side_effects=True, vmem_limit_bytes=24 * 1024 * 1024
        ),
    )(
        *(
            pltpu.with_memory_space_constraint(v, pltpu.HBM)
            for v in (owner_table.reshape(1, NB), pool_map, grads, momentum)
        )
    )
    return written(results)


def solution(mesh, sizes=(4, 8, 8, 16)):
    in_specs = (P("tp", None, "fsdp"), P("tp", None, "fsdp"), P("tp", None), P("tp", None))
    out_specs = (P("tp", None, "fsdp"), P("tp", None, "fsdp"), P("tp", "fsdp"))
    return jax.shard_map(
        functools.partial(local, sizes), mesh=mesh, in_specs=in_specs, out_specs=out_specs, check_vma=False
    )
```

```python
import functools
import math

import jax
import jax.numpy as jnp
from jax import lax
from jax.experimental import pallas as pl
from jax.experimental.pallas import tpu as pltpu
from jax.sharding import PartitionSpec as P

ITERS = 3
momentum_rate = 0.95
step_size = 0.8
epsilon = 1e-07
poly_linear = 3.4445
poly_cubic = -4.775
poly_quintic = 2.0315

H = 128
PACKED = H + 8
MESH = pl.DeviceIdType.MESH


def masks():
    row = lax.broadcasted_iota(jnp.int32, (H, H), 0)
    col = lax.broadcasted_iota(jnp.int32, (H, H), 1)
    return row >= col, row == col


def put_packed(ref, a, b):
    low, diag = masks()
    ref[0:H, :] = jnp.where(low, a, b)
    last = jnp.sum(jnp.where(diag, b, 0.0), axis=0, keepdims=True)
    ref[H:PACKED, :] = jnp.broadcast_to(last, (8, H))


def get_packed(ref):
    low, diag = masks()
    both = ref[0:H, :]
    other = both.T
    last = jnp.broadcast_to(ref[H : H + 1, :], (H, H))
    a = jnp.where(low, both, other)
    b = jnp.where(diag, last, jnp.where(low, other, both))
    return a, b


def halves(v):
    high = v.astype(jnp.bfloat16)
    return high, (v - high.astype(jnp.float32)).astype(jnp.bfloat16)


def dot32(a, b):
    (ah, al), (bh, bl) = halves(a), halves(b)
    return jnp.dot(
        jnp.concatenate([ah, al, ah], axis=1),
        jnp.concatenate([bh, bh, bl], axis=0),
        preferred_element_type=jnp.float32,
    )


def newton_schulz(grams):
    _, diag = masks()
    identity = jnp.where(diag, 1.0, 0.0)
    inverses, gs, qs = [], [], [None] * len(grams)
    for g in grams:
        squares = jnp.sum(jnp.where(diag, g, 0.0), keepdims=True)
        inverse = 1.0 / (jnp.sqrt(squares) + epsilon)
        inverses.append(inverse)
        gs.append(g * (inverse * inverse))
    for it in range(ITERS):
        g2 = [dot32(g, g) for g in gs]
        ms = [poly_linear * identity + poly_cubic * g + poly_quintic * s for g, s in zip(gs, g2)]
        if it < ITERS - 1:
            right = [dot32(g, m) for g, m in zip(gs, ms)]
        qs = [m if it == 0 else dot32(m, q) for m, q in zip(ms, qs)]
        if it < ITERS - 1:
            gs = [dot32(m, r) for m, r in zip(ms, right)]
    return [q * inverse for q, inverse in zip(qs, inverses)]


def kernel(
    sizes,
    owner_hbm,
    pool_hbm,
    g_hbm,
    m_hbm,
    nm_ref,
    out_ref,
    slot_ref,
    owner_ref,
    pool_ref,
    gbuf,
    mbuf,
    yq,
    yr,
    pk,
    r0,
    s1,
    r1,
    s2,
    r2,
    rd,
    s3,
    sd,
    gram,
    qall,
    t0,
    t0r,
    t1,
    t1r,
    t2,
    t2r,
    in_sem,
    z_send,
    z_recv,
    c_send,
    c_recv,
    x_send,
    x_recv,
    y_send,
    y_recv,
    t_send,
    t_recv,
    w_send,
    w_recv,
    a_send,
    a_recv,
    b_send,
    b_recv,
):
    NX, NY, NZ, NB = sizes
    NK = 2 * NX
    CH = H // NY
    f = lax.axis_index("fsdp")
    z = lax.axis_index("tp")
    k = lax.rem(f, NK)
    y = lax.div(f, NK)
    x = lax.div(k, 2)
    c = lax.rem(k, 2)
    plane = lax.rem(k + NZ - z, NZ)

    def dev(yy, xx, cc, zz):
        return ((yy * NX + xx) * 2 + cc, zz)

    partner = dev(y, x, 1 - c, z)

    def xdev(d):
        return dev(y, lax.rem(x + d, NX), c, z)

    def ydev(d):
        return dev(lax.rem(y + d, NY), x, c, z)

    def zdev(d):
        return dev(y, x, c, lax.rem(z + d, NZ))

    def wdev(d):
        return (lax.rem(y + d, NY) * NK + k, plane)

    def remote(src, dst, send, recv, device):
        return pltpu.make_async_remote_copy(
            src_ref=src, dst_ref=dst, send_sem=send, recv_sem=recv, device_id=device, device_id_type=MESH
        )

    own_copy = pltpu.make_async_copy(owner_hbm, owner_ref, in_sem.at[8])
    pool_copy = pltpu.make_async_copy(pool_hbm, pool_ref, in_sem.at[9])
    own_copy.start()
    pool_copy.start()
    CHUNKS = 4
    per = NB // CHUNKS
    loads = []
    for i in range(CHUNKS):
        part = pl.ds(i * per, per)
        lg = pltpu.make_async_copy(g_hbm.at[part], gbuf.at[part], in_sem.at[2 * i])
        lm = pltpu.make_async_copy(m_hbm.at[part], mbuf.at[part], in_sem.at[2 * i + 1])
        lg.start()
        lm.start()
        loads.append((lg, lm))

    barrier = pltpu.get_barrier_semaphore()

    def greet(device):
        pl.semaphore_signal(barrier, inc=1, device_id=device, device_id_type=MESH)

    for d in range(1, NZ):
        greet(zdev(d))
    for d in range(1, NY):
        greet(ydev(d))
    for d in range(1, NX):
        greet(xdev(d))
    greet(partner)

    own_copy.wait()
    pool_copy.wait()
    codes = [pool_ref[0, j] for j in range(NB)]

    def source(q):
        at = jnp.int32(0)
        for j in range(1, NB):
            at = jnp.where(codes[j] == q, j, at)
        return at

    left, right, far = lax.rem(x + NX - 1, NX), lax.rem(x + 1, NX), lax.rem(x + 2, NX)
    order = [far, left, right, x]
    blocks = {}
    for whose, core in (("theirs", 1 - c), ("ours", c)):
        for i, at in enumerate(order):
            p = lax.rem(2 * at + core + NZ - z, NZ)
            blocks[whose, i] = (p, [source(2 * p), source(2 * p + 1)])

    for pair in loads:
        for cp in pair:
            cp.wait()

    def nesterov(j):
        grad = gbuf[j].astype(jnp.float32)
        velocity = momentum_rate * mbuf[j].astype(jnp.float32) + grad
        return velocity, (grad + momentum_rate * velocity).astype(jnp.bfloat16)

    def over_z(d):
        to = lax.rem(z + d, NZ)
        return remote(
            yq.at[pl.ds(2 * to, 2)], yr.at[pl.ds(2 * z, 2)], z_send.at[d], z_recv.at[d], (f, to)
        )

    mine = pltpu.make_async_copy(yq.at[pl.ds(2 * z, 2)], yr.at[pl.ds(2 * z, 2)], z_recv.at[0])

    def send_y(p):
        d = lax.rem(p + NZ - z, NZ)

        @pl.when(d != 0)
        def _():
            over_z(d).start()

        @pl.when(d == 0)
        def _():
            mine.start()

    def make_pair(whose, i):
        core, at = (c if whose == "ours" else 1 - c), order[i]
        p, taken = blocks[whose, i]
        grams = []
        for e in range(2):
            q = 2 * p + e
            _, value = nesterov(taken[e])
            yq[q] = value
            wide = value.astype(jnp.float32)
            t0[pl.ds(q, 1), :] = jnp.sum(wide * wide, axis=0, keepdims=True)
            grams.append(
                lax.dot_general(value, value, (((1,), (1,)), ((), ())), preferred_element_type=jnp.float32)
            )
        put_packed(pk.at[core, at], *grams)

    sent = []

    def go(copy):
        copy.start()
        sent.append(copy)
        return copy

    cc = []
    for i, at in enumerate(order):
        make_pair("theirs", i)
        if i == 0:
            pl.semaphore_wait(barrier, (NZ - 1) + (NY - 1) + (NX - 1) + 1)
        cc.append(go(remote(pk.at[1 - c, at], r0.at[at], c_send.at[i], c_recv.at[i], partner)))
        send_y(blocks["theirs", i][0])
    for i in range(NX):
        make_pair("ours", i)
        send_y(blocks["ours", i][0])
    ct = go(remote(t0, t0r, c_send.at[NX], c_recv.at[NX], partner))

    upper, lower = pl.ds(0, H // 2), pl.ds(H // 2, PACKED - H // 2)
    to_right = {"device": dev(y, right, c, z)}
    to_left = {"device": dev(y, left, c, z)}
    xc = []
    for i, d in enumerate((2, 3, 1)):
        cc[i].wait_recv()
        at = order[i]
        s1[at] = pk[c, at] + r0[at]
        xc.append(go(remote(s1.at[at], r1.at[d - 1], x_send.at[d], x_recv.at[d], xdev(d))))
    ct.wait_recv()
    t1[...] = t0[...] + t0r[...]
    tx = [go(remote(t1, t1r.at[d - 1], t_send.at[d], t_recv.at[d], xdev(d))) for d in range(1, NX)]
    cc[3].wait_recv()
    s1[x] = pk[c, x] + r0[x]

    for j in range(NB):
        nm_ref[j] = nesterov(j)[0].astype(jnp.bfloat16)

    for cp in xc:
        cp.wait_recv()
    s2[...] = s1[x] + r1[0] + r1[1] + r1[2]
    yc, yd = [], []
    for d in sorted(range(1, NY), key=lambda d: -min(d, NY - d)):
        to = lax.rem(y + d, NY)
        rows = pl.ds(pl.multiple_of(to * CH, CH), CH)
        yc.append(go(remote(s2.at[rows], r2.at[d - 1], y_send.at[d], y_recv.at[d], ydev(d))))
    for d in range(1, NY):
        yd.append(go(remote(s2.at[pl.ds(H, 8)], rd.at[d - 1], y_send.at[NY + d], y_recv.at[NY + d], ydev(d))))
    for cp in tx:
        cp.wait_recv()
    ttotal = t1[...]
    for d in range(1, NX):
        ttotal = ttotal + t1r[d - 1]
    t2[...] = ttotal
    ty = [go(remote(t2, t2r.at[d - 1], t_send.at[NX + d], t_recv.at[NX + d], ydev(d))) for d in range(1, NY)]

    for cp in yc:
        cp.wait_recv()
    total = s2[pl.ds(pl.multiple_of(y * CH, CH), CH), :]
    for d in range(1, NY):
        total = total + r2[d - 1]
    s3[...] = total
    own_rows = pl.ds(pl.multiple_of(y * CH, CH), CH)
    wc = []
    for d in sorted(range(1, NY), key=lambda d: -min(d, NY - d)):
        wc.append(go(remote(s3, gram.at[own_rows], w_send.at[d], w_recv.at[d], wdev(d))))
    for cp in yd:
        cp.wait_recv()
    total = s2[pl.ds(H, 8), :]
    for d in range(1, NY):
        total = total + rd[d - 1]
    sd[...] = total
    w0 = remote(s3, gram.at[own_rows], w_send.at[0], w_recv.at[0], wdev(0))
    w1 = remote(sd, gram.at[pl.ds(H, 8)], w_send.at[NY], w_recv.at[NY], wdev(0))
    l0 = pltpu.make_async_copy(s3, gram.at[own_rows], w_recv.at[0])
    l1 = pltpu.make_async_copy(sd, gram.at[pl.ds(H, 8)], w_recv.at[NY])

    @pl.when(plane != z)
    def _():
        w0.start()
        w1.start()

    @pl.when(plane == z)
    def _():
        l0.start()
        l1.start()

    for cp in ty:
        cp.wait_recv()
    ttotal = t2[...]
    for d in range(1, NY):
        ttotal = ttotal + t2r[d - 1]
    t2r[NY - 1] = ttotal
    count = jnp.int32(0)
    picked = [jnp.zeros((1, H), jnp.float32), jnp.zeros((1, H), jnp.float32)]
    for j in range(NB):
        same = jnp.where(owner_ref[0, j] == f, 1, 0)
        line = t2r[NY - 1, pl.ds(codes[j], 1), :]
        for s in range(2):
            weight = jnp.where(count == s, same, 0).astype(jnp.float32)
            picked[s] = picked[s] + line * weight
        count = count + same
    lane = lax.broadcasted_iota(jnp.int32, (1, 2), 1)
    sums = [jnp.sum(v, axis=1, keepdims=True) for v in picked]
    elements = H * H * NK * NY
    slot_ref[...] = jnp.sqrt(jnp.where(lane == 0, sums[0], sums[1]) / elements)

    for cp in wc:
        cp.wait_recv()
    l0.wait()
    l1.wait()
    a, b = newton_schulz(list(get_packed(gram)))
    put_packed(qall.at[k], a, b)

    xa = {}
    for d in (2, 1, 3):
        xa[d] = go(remote(qall.at[k], qall.at[k], a_send.at[d], a_recv.at[d], xdev(d)))
    b_own = go(remote(qall.at[k], qall.at[k], b_send.at[0], b_recv.at[0], partner))

    mine.wait()
    for d in range(1, NZ):
        over_z(d).wait_recv()
    factor = step_size * 0.2 * math.sqrt(H * NK * NY)

    def apply(at):
        slot = lax.rem(at + NZ - z, NZ)
        for e, q in enumerate(get_packed(qall.at[at])):
            high = q.astype(jnp.bfloat16)
            rest = (q - high.astype(jnp.float32)).astype(jnp.bfloat16)
            value = yr[2 * slot + e]
            ortho = jnp.dot(
                jnp.concatenate([high, rest], axis=1),
                jnp.concatenate([value, value], axis=0),
                preferred_element_type=jnp.float32,
            ).astype(jnp.bfloat16)
            out_ref[2 * slot + e] = (-factor * ortho.astype(jnp.float32)).astype(jnp.bfloat16)

    def across(at, i):
        return go(remote(qall.at[at], qall.at[at], b_send.at[i], b_recv.at[i], partner))

    apply(k)
    b_own.wait_recv()
    apply(2 * x + 1 - c)
    fwd = {}
    for d in (1, 3, 2):
        xa[d].wait_recv()
        at = 2 * lax.rem(x + NX - d, NX) + c
        fwd[d] = go(remote(qall.at[at], qall.at[at], b_send.at[d], b_recv.at[d], partner))
        apply(at)
    for d in (1, 3, 2):
        fwd[d].wait_recv()
        apply(2 * lax.rem(x + NX - d, NX) + 1 - c)

    for cp in sent:
        cp.wait_send()
    for d in range(1, NZ):
        over_z(d).wait_send()

    @pl.when(plane != z)
    def _():
        w0.wait_send()
        w1.wait_send()


def writer(*refs):
    copies = [pltpu.make_async_copy(refs[i], refs[3 + i], refs[6].at[i]) for i in range(3)]
    for cp in copies:
        cp.start()
    for cp in copies:
        cp.wait()


def written(results):
    vmem = pl.BlockSpec(memory_space=pltpu.VMEM)
    return pl.pallas_call(
        writer,
        out_shape=tuple(jax.ShapeDtypeStruct(v.shape, v.dtype) for v in results),
        in_specs=[vmem] * 3,
        out_specs=(pl.BlockSpec(memory_space=pltpu.HBM),) * 3,
        scratch_shapes=[pltpu.SemaphoreType.DMA((3,))],
        compiler_params=pltpu.CompilerParams(vmem_limit_bytes=8 * 1024 * 1024),
    )(*results)


def local(sizes, grads, momentum, owner_table, pool_map):
    NX, NY, NZ, NB = sizes
    NK = 2 * NX
    f32, bf16 = jnp.float32, jnp.bfloat16
    dma = pltpu.SemaphoreType.DMA
    hbm = pl.BlockSpec(memory_space=pltpu.HBM)
    scratch = [
        pltpu.SMEM((1, NB), jnp.int32),
        pltpu.SMEM((1, NB), jnp.int32),
        pltpu.VMEM((NB, H, H), bf16),
        pltpu.VMEM((NB, H, H), bf16),
        pltpu.VMEM((NB, H, H), bf16),
        pltpu.VMEM((NB, H, H), bf16),
        pltpu.VMEM((2, NX, PACKED, H), f32),
        pltpu.VMEM((NX, PACKED, H), f32),
        pltpu.VMEM((NX, PACKED, H), f32),
        pltpu.VMEM((NX - 1, PACKED, H), f32),
        pltpu.VMEM((PACKED, H), f32),
        pltpu.VMEM((NY - 1, H // NY, H), f32),
        pltpu.VMEM((NY - 1, 8, H), f32),
        pltpu.VMEM((H // NY, H), f32),
        pltpu.VMEM((8, H), f32),
        pltpu.VMEM((PACKED, H), f32),
        pltpu.VMEM((NK, PACKED, H), f32),
        pltpu.VMEM((NB, H), f32),
        pltpu.VMEM((NB, H), f32),
        pltpu.VMEM((NB, H), f32),
        pltpu.VMEM((NX - 1, NB, H), f32),
        pltpu.VMEM((NB, H), f32),
        pltpu.VMEM((NY, NB, H), f32),
        dma((10,)),
        dma((NZ,)),
        dma((NZ,)),
        dma((NX + 1,)),
        dma((NX + 1,)),
        dma((6,)),
        dma((6,)),
        dma((2 * NY,)),
        dma((2 * NY,)),
        dma((NX + NY,)),
        dma((NX + NY,)),
        dma((NY + 1,)),
        dma((NY + 1,)),
        dma((6,)),
        dma((6,)),
        dma((NX,)),
        dma((NX,)),
    ]
    results = pl.pallas_call(
        functools.partial(kernel, sizes),
        out_shape=(
            jax.ShapeDtypeStruct(grads.shape, bf16),
            jax.ShapeDtypeStruct(grads.shape, bf16),
            jax.ShapeDtypeStruct((1, 2), f32),
        ),
        in_specs=[hbm] * 4,
        out_specs=(pl.BlockSpec(memory_space=pltpu.VMEM),) * 3,
        scratch_shapes=scratch,
        compiler_params=pltpu.CompilerParams(
            collective_id=0, has_side_effects=True, vmem_limit_bytes=24 * 1024 * 1024
        ),
    )(
        *(
            pltpu.with_memory_space_constraint(v, pltpu.HBM)
            for v in (owner_table.reshape(1, NB), pool_map, grads, momentum)
        )
    )
    return written(results)


def solution(mesh, sizes=(4, 8, 8, 16)):
    in_specs = (P("tp", None, "fsdp"), P("tp", None, "fsdp"), P("tp", None), P("tp", None))
    out_specs = (P("tp", None, "fsdp"), P("tp", None, "fsdp"), P("tp", "fsdp"))
    return jax.shard_map(
        functools.partial(local, sizes), mesh=mesh, in_specs=in_specs, out_specs=out_specs, check_vma=False
    )
```
